256 devices in a mesh: samp: 32 (over y, z_hi, x), tile: 8 (over z_lo, core).
Axes of the slice: x: 4, y: 4, z: 8 (z_hi: 2, z_lo: 4; z = z_hi * 4 + z_lo), core: 2. Of those that a mesh axis runs over, the one named last changes fastest.
Arguments:
- traits: bfloat16 [32768, 1024], P('samp'), may hold values from -300 to 300
- covariates: bfloat16 [32768, 32], P('samp'), may hold values from -6 to 6
- genotypes: int32 [32768, 2048], P('samp', 'tile'), may hold values from 0 to 2
- shuffles: int32 [6, 32768], P(None, 'samp'), may hold values from 0 to 32767, as said below
Outputs:
- observed: float32 [1024, 2048], P('samp', 'tile')
- perm_max: float32 [6, 1024], P(None, 'samp')
The draws below stay inside these ranges and needn't reach their ends.
Inputs may be any that keep to these rules, and one draw needn't show every extreme that they name: Row p of shuffles maps each aligned block of 1024 samples one to one onto the same block's samples.
All inputs are finite; a program needn't handle non-finite values.
Results may differ from the reference program's by a relative error of at most 0.0045.
Values sent between devices are 32-bit elements; how exact they have to be, the bound alone decides.
A program may use at most 64 MiB of HBM per device.

```python
import math
import jax
import jax.numpy as jnp
from jax import lax

SAMP_DEV = 1024
E = 1024
C = 32
PERMS = 6
SAMPLES = 32768
VARIANTS = 2048


def covariate_base(key):
    values = jax.random.normal(jax.random.fold_in(key, 11), (SAMPLES, C), jnp.float32)
    return jnp.clip(values, -6.0, 6.0)


def draw_covariates(key, part):
    return covariate_base(key).astype(jnp.bfloat16)


def draw_traits(key, part):
    base = covariate_base(key)
    key_load, key_mean, key_noise, key_cols = jax.random.split(jax.random.fold_in(key, 23), 4)
    loading = jax.random.normal(key_load, (C, E), jnp.float32) / math.sqrt(C)
    means = 2.0 * jnp.clip(jax.random.normal(key_mean, (E,), jnp.float32), -4.0, 4.0)
    col_scale = jnp.exp(jax.random.uniform(key_cols, (E,), jnp.float32, 0.0, math.log(10.0)))
    position = jnp.arange(SAMPLES, dtype=jnp.float32) / SAMPLES
    noise = jnp.clip(jax.random.normal(key_noise, (SAMPLES, E), jnp.float32), -5.0, 5.0)
    row_scale = 1.0 + 2.0 * position
    fitted = jnp.dot(base, loading, precision=lax.Precision.HIGHEST)
    values = (means[None, :] + fitted + noise) * row_scale[:, None] * col_scale[None, :]
    return jnp.clip(values, -300.0, 300.0).astype(jnp.bfloat16)


def draw_genotypes(key, part):
    key_freq, key_first, key_second = jax.random.split(jax.random.fold_in(key, 37), 3)
    freq = jax.random.randint(key_freq, (1, VARIANTS), 5, 96)
    first = (jax.random.randint(key_first, (SAMPLES, VARIANTS), 0, 100) < freq).astype(jnp.int32)
    second = (jax.random.randint(key_second, (SAMPLES, VARIANTS), 0, 100) < freq).astype(jnp.int32)
    return first + second


def draw_shuffles(key, part):
    blocks = SAMPLES // SAMP_DEV
    keys = jax.random.split(jax.random.fold_in(key, 41), PERMS * blocks)
    orders = jax.vmap(lambda one_key: jax.random.permutation(one_key, SAMP_DEV))(keys).astype(jnp.int32)
    offsets = jnp.arange(blocks, dtype=jnp.int32) * SAMP_DEV
    orders = orders.reshape(PERMS, blocks, SAMP_DEV) + offsets[None, :, None]
    return orders.reshape(PERMS, SAMPLES).astype(jnp.int32)


def setup_inputs(seed: int = 0) -> dict:
    key_of = jax.random.split(jax.random.key(seed), 5)
    return {
        "traits": draw_traits(jax.random.fold_in(key_of[4], 71), 0),
        "covariates": draw_covariates(jax.random.fold_in(key_of[4], 71), 0),
        "genotypes": draw_genotypes(jax.random.fold_in(key_of[4], 71), 0),
        "shuffles": draw_shuffles(jax.random.fold_in(key_of[4], 71), 0),
    }


epsilon = 1e-05

def cholesky_solve(factor, rhs):
    first = lax.linalg.triangular_solve(factor, rhs, left_side=True, lower=True)
    return lax.linalg.triangular_solve(factor, first, left_side=True, lower=True, transpose_a=True)

def reference(traits, covariates, genotypes, shuffles):
    ones = jnp.ones((covariates.shape[0], 1), jnp.bfloat16)
    design = jnp.concatenate([ones, covariates], axis=1)
    dosage = genotypes.astype(jnp.bfloat16)
    gram = jnp.dot(design.T.astype(jnp.float32), design.astype(jnp.float32), preferred_element_type=jnp.float32)
    xty = jnp.dot(design.T.astype(jnp.float32), traits.astype(jnp.float32), preferred_element_type=jnp.float32)
    xtg = jnp.dot(design.T.astype(jnp.float32), dosage.astype(jnp.float32), preferred_element_type=jnp.float32)
    factor = jnp.linalg.cholesky(gram)
    coef_traits = cholesky_solve(factor, xty).astype(jnp.bfloat16)
    coef_geno = cholesky_solve(factor, xtg).astype(jnp.bfloat16)
    resid_traits = traits.astype(jnp.float32) - jnp.dot(design.astype(jnp.float32), coef_traits.astype(jnp.float32), preferred_element_type=jnp.float32)
    resid_geno = dosage.astype(jnp.float32) - jnp.dot(design.astype(jnp.float32), coef_geno.astype(jnp.float32), preferred_element_type=jnp.float32)
    mean_traits = lax.optimization_barrier(jnp.sum(resid_traits * resid_traits, axis=0)) / SAMPLES
    mean_geno = lax.optimization_barrier(jnp.sum(resid_geno * resid_geno, axis=0)) / SAMPLES
    rt_rows = resid_traits.astype(jnp.bfloat16)
    rg_rows = resid_geno.astype(jnp.bfloat16)
    scale_traits = lax.rsqrt(mean_traits + epsilon)
    scale_geno = lax.rsqrt(mean_geno + epsilon)
    factor_z = math.sqrt(SAMPLES - C - 2) / SAMPLES

    def scores_of(trait_rows):
        cross = jnp.dot(trait_rows.T.astype(jnp.float32), rg_rows.astype(jnp.float32), preferred_element_type=jnp.float32)
        return cross * scale_traits[:, None] * scale_geno[None, :] * factor_z
    observed = scores_of(rt_rows)

    def one_perm(order):
        shuffled = jnp.take(rt_rows, order.astype(jnp.int32), axis=0)
        return lax.optimization_barrier(jnp.max(jnp.abs(scores_of(shuffled)), axis=1))
    perm_max = lax.map(one_perm, shuffles)
    return (observed, perm_max)
```

```python
import functools
import math

import jax
import jax.numpy as jnp
from jax import lax
from jax.experimental import pallas as pl
from jax.experimental.pallas import tpu as pltpu
from jax.sharding import PartitionSpec as P

C = 32


epsilon = 1e-05
MESH = pl.DeviceIdType.MESH


def filled_up(lines, count):
    spare = -len(lines) % count
    return jnp.pad(lines, [(0, spare)] + [(0, 0)] * (lines.ndim - 1))


def joined_along(blocks, dim):
    lengths = list(blocks.shape[1:])
    lengths[dim] *= blocks.shape[0]
    return jnp.moveaxis(blocks, 0, dim).reshape(lengths)


def copy_for_each(value, axis):
    copies = jnp.broadcast_to(value, (lax.axis_size(axis), *value.shape))
    return lax.all_to_all(copies, axis, split_axis=0, concat_axis=0, tiled=True)


def gathered_copies(value, axis, dim):
    return joined_along(copy_for_each(value, axis), dim)


def in_blocks(value, dim, count):
    lengths = value.shape
    blocks = value.reshape(*lengths[:dim], count, lengths[dim] // count, *lengths[dim + 1 :])
    return jnp.moveaxis(blocks, dim, 0)


def sum_at_owner(value, axis, dim):
    count = lax.axis_size(axis)
    blocks = lax.all_to_all(in_blocks(value, dim, count), axis, 0, 0, tiled=True)
    return jnp.sum(blocks, axis=0)


def total_of(value, axes):
    padded = filled_up(value, lax.axis_size(axes))
    whole = gathered_copies(sum_at_owner(padded, axes, 0), axes, 0)
    return lax.slice_in_dim(whole, 0, len(value)).reshape(value.shape)


def together(arrays, axis):
    line, at, outs = (jnp.concatenate([a.reshape(-1) for a in arrays]), 0, [])
    running = total_of(line, axis)
    for a in arrays:
        outs.append(running[at : at + a.size].reshape(a.shape))
        at += a.size
    return tuple(outs)


def over_copies(value, axis):
    everything = copy_for_each(value, axis)
    return jnp.sum(everything, axis=0)


def packed_total(arrays, axis):
    ends = [0]
    for a in arrays:
        ends.append(ends[-1] + a.size)
    running = over_copies(jnp.concatenate([a.ravel() for a in arrays]), axis)
    return tuple((running[b:e].reshape(a.shape) for a, b, e in zip(arrays, ends, ends[1:])))


def cholesky_solve(factor, rhs):
    first = lax.linalg.triangular_solve(factor, rhs, left_side=True, lower=True)
    return lax.linalg.triangular_solve(factor, first, left_side=True, lower=True, transpose_a=True)


def cross_local(left, right):
    return lax.dot_general(
        left, right, (((0,), (0,)), ((), ())), preferred_element_type=jnp.float32
    )


def scan_kernel(
    yt_ref, g_ref, order_ref, st_ref, sg_ref, obs_ref, peak_ref,
    q_ref, part, in1, mid, in2, low, inz, pm, pmin,
    send1, recv1, send2, recv2, sendz, recvz, sendt, recvt,
):
    perms = order_ref.shape[0]
    mats = perms + 1
    s = lax.axis_index("samp")
    t = lax.axis_index("tile")
    x = lax.rem(s, 4)
    zh = lax.rem(s // 4, 2)
    y = s // 8
    base = s * yt_ref.shape[1]

    def at_x(v):
        return s - x + lax.rem(v, 4)

    def at_y(v):
        return lax.rem(v, 4) * 8 + lax.rem(s, 8)

    z_peer = s + 4 - 8 * zh
    place = (x, y)
    peers = ((at_x(x + 1), at_x(x + 3)), (at_y(y + 1), at_y(y + 3)))

    barrier = pltpu.get_barrier_semaphore()
    for peer in (*peers[0], *peers[1], z_peer):
        pl.semaphore_signal(barrier, inc=1, device_id={"samp": peer}, device_id_type=MESH)
    for d in range(1, 8):
        pl.semaphore_signal(
            barrier, inc=1, device_id={"tile": lax.rem(t + d, 8)}, device_id_type=MESH
        )
    pl.semaphore_wait(barrier, 12)

    def remote(src, dst, send, recv, peer):
        return pltpu.make_async_remote_copy(
            src_ref=src, dst_ref=dst, send_sem=send, recv_sem=recv,
            device_id={"samp": peer}, device_id_type=MESH,
        )

    def first_copy(h, m, k):
        c = place[h]
        blk = lax.rem(c + (2, 1, 2, 3, 1, 3)[k], 4)
        uv = (0, 1, 1, 0, 0, 1)[k]
        src = part.at[h, m, blk, uv]
        if k >= 4:
            src = in1.at[h, m, 0 if k == 4 else 2]
        return remote(
            src, in1.at[h, m, k], send1.at[h, m, k], recv1.at[h, m, k],
            peers[h][(0, 0, 1, 1, 0, 1)[k]],
        )

    def second_copy(h, m, k):
        c = place[1 - h]
        blk = lax.rem(c + (2, 1, 2, 3, 1, 3)[k], 4)
        uv = (0, 1, 1, 0, 0, 1)[k]
        src = mid.at[h, m, blk, uv]
        if k >= 4:
            src = in2.at[h, m, 0 if k == 4 else 2]
        return remote(
            src, in2.at[h, m, k], send2.at[h, m, k], recv2.at[h, m, k],
            peers[1 - h][(0, 0, 1, 1, 0, 1)[k]],
        )

    def z_copy(h, m):
        return remote(
            low.at[h, m, 1 - zh], inz.at[h, m], sendz.at[h, m], recvz.at[h, m], z_peer
        )

    def compute(m, rows_ref):
        def block(yb, carry):
            lines = yt_ref[pl.ds(pl.multiple_of(yb * 256, 256), 256), :]
            out = jnp.dot(lines, rows_ref[...], preferred_element_type=jnp.float32)
            for z in range(2):
                for xb in range(4):
                    at = (z * 4 + xb) * 32
                    part[0, m, xb, z, yb] = out[at : at + 32, :128]
                    part[1, m, yb, z, xb] = out[at : at + 32, 128:]
            return carry

        lax.fori_loop(0, 4, block, 0)

    def permute(m):
        order = order_ref[pl.ds(m - 1, 1), :] - base

        def block(jb, carry):
            target = lax.broadcasted_iota(jnp.int32, (256, order.shape[1]), 0) + jb * 256
            hot = jnp.where(target == order, 1.0, 0.0).astype(jnp.bfloat16)
            rows = jnp.dot(hot, g_ref[...], preferred_element_type=jnp.float32)
            q_ref[pl.ds(pl.multiple_of(jb * 256, 256), 256), :] = rows.astype(jnp.bfloat16)
            return carry

        lax.fori_loop(0, 4, block, 0)

    def stage1(m):
        for k in (0, 2, 1, 3):
            for h in range(2):
                first_copy(h, m, k).start()

    def stage2(m):
        for h in range(2):
            c = place[h]
            first_copy(h, m, 0).wait_recv()
            in1[h, m, 0] = in1[h, m, 0] + part[h, m, lax.rem(c + 1, 4), 0]
            first_copy(h, m, 4).start()
            first_copy(h, m, 2).wait_recv()
            in1[h, m, 2] = in1[h, m, 2] + part[h, m, lax.rem(c + 3, 4), 1]
            first_copy(h, m, 5).start()

    def stage3(m):
        for h in range(2):
            c = place[h]
            for k in (1, 3, 4, 5):
                first_copy(h, m, k).wait_recv()
            mid[h, m, :, 0] = part[h, m, c, 0] + in1[h, m, 3] + in1[h, m, 4]
            mid[h, m, :, 1] = part[h, m, c, 1] + in1[h, m, 1] + in1[h, m, 5]
            for k in (0, 2, 1, 3):
                second_copy(h, m, k).start()

    def stage4(m):
        for h in range(2):
            c = place[1 - h]
            second_copy(h, m, 0).wait_recv()
            in2[h, m, 0] = in2[h, m, 0] + mid[h, m, lax.rem(c + 1, 4), 0]
            second_copy(h, m, 4).start()
            second_copy(h, m, 2).wait_recv()
            in2[h, m, 2] = in2[h, m, 2] + mid[h, m, lax.rem(c + 3, 4), 1]
            second_copy(h, m, 5).start()

    def stage5(m):
        for h in range(2):
            c = place[1 - h]
            for k in (1, 3, 4, 5):
                second_copy(h, m, k).wait_recv()
            low[h, m, 0] = mid[h, m, c, 0] + in2[h, m, 3] + in2[h, m, 4]
            low[h, m, 1] = mid[h, m, c, 1] + in2[h, m, 1] + in2[h, m, 5]
            z_copy(h, m).start()

    def owned(m):
        outs = []
        for h in range(2):
            z_copy(h, m).wait_recv()
            total = low[h, m, zh] + inz[h, m]
            outs.append(total * st_ref[...] * sg_ref[:, h * 128 : (h + 1) * 128])
        return outs

    lane = lax.broadcasted_iota(jnp.int32, (32, 128), 1)

    def stage6(m):
        left, right = owned(m)
        peak = jnp.max(jnp.maximum(jnp.abs(left), jnp.abs(right)), axis=1, keepdims=True)
        pm[...] = jnp.where(lane == m - 1, peak, pm[...])

    pm[...] = jnp.zeros_like(pm)
    compute(0, g_ref)
    stage1(0)

    def step(i, carry):
        @pl.when(i < mats)
        def _():
            permute(i)
            compute(i, q_ref)
            stage1(i)

        for lag, stage in ((1, stage2), (2, stage3), (3, stage4), (4, stage5)):
            @pl.when((i >= lag) & (i < mats + lag))
            def _(stage=stage, lag=lag):
                stage(i - lag)

        @pl.when((i >= 6) & (i < mats + 5))
        def _():
            stage6(i - 5)

        @pl.when(i == 5)
        def _():
            left, right = owned(0)
            obs_ref[:, :128] = left
            obs_ref[:, 128:] = right

        return carry

    lax.fori_loop(1, mats + 5, step, 0)

    def tile_copy(d):
        return pltpu.make_async_remote_copy(
            src_ref=pm, dst_ref=pmin.at[d - 1], send_sem=sendt.at[d - 1],
            recv_sem=recvt.at[d - 1], device_id={"tile": lax.rem(t + d, 8)},
            device_id_type=MESH,
        )

    for d in range(1, 8):
        tile_copy(d).start()

    def drain(m, carry):
        for h in range(2):
            for k in range(6):
                first_copy(h, m, k).wait_send()
                second_copy(h, m, k).wait_send()
            z_copy(h, m).wait_send()
        return carry

    lax.fori_loop(0, mats, drain, 0)
    best = pm[...]
    for d in range(1, 8):
        tile_copy(d).wait_recv()
        best = jnp.maximum(best, pmin[d - 1])
    peak_ref[...] = best
    for d in range(1, 8):
        tile_copy(d).wait_send()


def scan(yt, g, order, st, sg):
    perms = order.shape[0]
    mats = perms + 1
    vmem = pl.BlockSpec(memory_space=pltpu.VMEM)
    f32 = jnp.float32
    dma = pltpu.SemaphoreType.DMA
    return pl.pallas_call(
        scan_kernel,
        out_shape=(
            jax.ShapeDtypeStruct((32, 256), f32),
            jax.ShapeDtypeStruct((32, 128), f32),
        ),
        in_specs=[vmem] * 5,
        out_specs=(vmem, vmem),
        scratch_shapes=[
            pltpu.VMEM(g.shape, jnp.bfloat16),
            pltpu.VMEM((2, mats, 4, 2, 4, 32, 128), f32),
            pltpu.VMEM((2, mats, 6, 4, 32, 128), f32),
            pltpu.VMEM((2, mats, 4, 2, 32, 128), f32),
            pltpu.VMEM((2, mats, 6, 32, 128), f32),
            pltpu.VMEM((2, mats, 2, 32, 128), f32),
            pltpu.VMEM((2, mats, 32, 128), f32),
            pltpu.VMEM((32, 128), f32),
            pltpu.VMEM((7, 32, 128), f32),
            dma((2, mats, 6)), dma((2, mats, 6)),
            dma((2, mats, 6)), dma((2, mats, 6)),
            dma((2, mats)), dma((2, mats)),
            dma((7,)), dma((7,)),
        ],
        compiler_params=pltpu.CompilerParams(
            collective_id=0, has_side_effects=True, vmem_limit_bytes=48 * 1024 * 1024
        ),
    )(yt, g, order, st, sg)


def shards(traits, covariates, genotypes, shuffles):
    groups = lax.axis_size("samp")
    own_index = lax.axis_index("samp")
    local_rows = traits.shape[0]
    samples = local_rows * groups
    share_rows = traits.shape[1] // groups
    ones = jnp.ones((local_rows, 1), jnp.bfloat16)
    design = jnp.concatenate([ones, covariates], axis=1)
    dosage = genotypes.astype(jnp.bfloat16)
    gram = cross_local(design, design)
    xty = cross_local(design, traits)
    xtg = cross_local(design, dosage)
    gram, xty, xtg = together((gram, xty, xtg), "samp")
    factor = jnp.linalg.cholesky(gram)
    coef_traits = cholesky_solve(factor, xty).astype(jnp.bfloat16)
    coef_geno = cholesky_solve(factor, xtg).astype(jnp.bfloat16)
    resid_traits = traits.astype(jnp.float32) - jnp.dot(
        design, coef_traits, preferred_element_type=jnp.float32
    )
    resid_geno = dosage.astype(jnp.float32) - jnp.dot(
        design, coef_geno, preferred_element_type=jnp.float32
    )
    sum_traits, sum_geno = packed_total(
        (jnp.sum(resid_traits * resid_traits, axis=0), jnp.sum(resid_geno * resid_geno, axis=0)),
        "samp",
    )
    mean_traits = sum_traits / samples
    mean_geno = sum_geno / samples
    rt_rows = resid_traits.astype(jnp.bfloat16)
    rg_rows = resid_geno.astype(jnp.bfloat16)
    scale_traits = lax.rsqrt(mean_traits + epsilon)
    scale_geno = lax.rsqrt(mean_geno + epsilon)
    factor_z = math.sqrt(samples - C - 2) / samples
    own_scale = lax.dynamic_slice_in_dim(scale_traits, own_index * share_rows, share_rows, 0)
    observed, peaks = scan(
        rt_rows.T, rg_rows, shuffles, own_scale[:, None] * factor_z, scale_geno[None, :]
    )
    return (observed, peaks[:, : shuffles.shape[0]].T)


def solution(mesh):
    placed = (P("samp", None), P("samp", None), P("samp", "tile"), P(None, "samp"))
    return jax.shard_map(
        shards,
        mesh=mesh,
        in_specs=placed,
        out_specs=(P("samp", "tile"), P(None, "samp")),
        check_vma=False,
    )
```

```python
import functools
import math

import jax
import jax.numpy as jnp
from jax import lax
from jax.experimental import pallas as pl
from jax.experimental.pallas import tpu as pltpu
from jax.sharding import PartitionSpec as P

C = 32


epsilon = 1e-05
MESH = pl.DeviceIdType.MESH
f32 = jnp.float32
bf16 = jnp.bfloat16


def exact_dot(a, b):
    return jnp.dot(a, b, preferred_element_type=f32, precision=lax.Precision.HIGHEST)


def across(a, b):
    return lax.dot_general(a, b, (((1,), (1,)), ((), ())), preferred_element_type=f32)


def iota(shape, dim):
    return lax.broadcasted_iota(jnp.int32, shape, dim)


def scan_kernel(
    y_ref, cov_ref, geno_ref, order_ref, obs_ref, peak_ref,
    yt, q, xt, tps, part, in1, mid, in2, low, inz, lowin, agu, tt,
    lhs, vst, corr, st_ref, sg_ref, pm, pmin,
    send1, recv1, send2, recv2, sendz, recvz, sendx, recvx, sendt, recvt,
    *, samples,
):
    perms = order_ref.shape[0]
    mats = perms + 1
    aux = mats
    rows = y_ref.shape[0]
    s = lax.axis_index("samp")
    t = lax.axis_index("tile")
    x = lax.rem(s, 4)
    zh = lax.rem(s // 4, 2)
    y = s // 8
    core = lax.rem(t, 2)
    zl = t // 2
    base = s * rows

    def at_x(v):
        return s - x + lax.rem(v, 4)

    def at_y(v):
        return lax.rem(v, 4) * 8 + lax.rem(s, 8)

    z_peer = s + 4 - 8 * zh
    place = (x, y)
    peers = ((at_x(x + 1), at_x(x + 3)), (at_y(y + 1), at_y(y + 3)))

    barrier = pltpu.get_barrier_semaphore()
    for peer in (*peers[0], *peers[1], at_y(y + 2), z_peer):
        pl.semaphore_signal(barrier, inc=1, device_id={"samp": peer}, device_id_type=MESH)
    for d in range(1, 8):
        pl.semaphore_signal(
            barrier, inc=1, device_id={"tile": lax.rem(t + d, 8)}, device_id_type=MESH
        )

    def remote(src, dst, send, recv, peer):
        return pltpu.make_async_remote_copy(
            src_ref=src, dst_ref=dst, send_sem=send, recv_sem=recv,
            device_id={"samp": peer}, device_id_type=MESH,
        )

    def to_tile(src, dst, k, d):
        return pltpu.make_async_remote_copy(
            src_ref=src, dst_ref=dst, send_sem=sendt.at[k, d - 1], recv_sem=recvt.at[k, d - 1],
            device_id={"tile": lax.rem(t + d, 8)}, device_id_type=MESH,
        )

    def first_copy(h, m, k):
        c = place[h]
        blk = lax.rem(c + (2, 1, 2, 3, 1, 3)[k], 4)
        uv = (0, 1, 1, 0, 0, 1)[k]
        src = part.at[h, m, blk, uv]
        if k >= 4:
            src = in1.at[h, m, 0 if k == 4 else 2]
        return remote(
            src, in1.at[h, m, k], send1.at[h, m, k], recv1.at[h, m, k],
            peers[h][(0, 0, 1, 1, 0, 1)[k]],
        )

    def second_copy(h, m, k):
        c = place[1 - h]
        blk = lax.rem(c + (2, 1, 2, 3, 1, 3)[k], 4)
        uv = (0, 1, 1, 0, 0, 1)[k]
        src = mid.at[h, m, blk, uv]
        if k >= 4:
            src = in2.at[h, m, 0 if k == 4 else 2]
        return remote(
            src, in2.at[h, m, k], send2.at[h, m, k], recv2.at[h, m, k],
            peers[1 - h][(0, 0, 1, 1, 0, 1)[k]],
        )

    def z_copy(h, m):
        return remote(
            low.at[h, m, 1 - zh], inz.at[h, m], sendz.at[h, m], recvz.at[h, m], z_peer
        )

    def compute(m):
        def block(yb, carry):
            lines = yt[pl.ds(pl.multiple_of(yb * 256, 256), 256), :]
            out = jnp.dot(lines, q[m, :, :256], preferred_element_type=f32)
            for z in range(2):
                for xb in range(4):
                    at = (z * 4 + xb) * 32
                    part[0, m, xb, z, yb] = out[at : at + 32, :128]
                    part[1, m, yb, z, xb] = out[at : at + 32, 128:]
            return carry

        lax.fori_loop(0, 4, block, 0)

    def permute(m):
        order = order_ref[pl.ds(m - 1, 1), :] - base

        def block(jb, carry):
            target = iota((256, rows), 0) + jb * 256
            hot = jnp.where(target == order, 1.0, 0.0).astype(bf16)
            moved = jnp.dot(hot, q[0], preferred_element_type=f32)
            q[m, pl.ds(pl.multiple_of(jb * 256, 256), 256), :] = moved.astype(bf16)
            return carry

        lax.fori_loop(0, 4, block, 0)

    def stage1(m, halves=(0, 1)):
        for k in (0, 2, 1, 3):
            for h in halves:
                first_copy(h, m, k).start()

    def stage2(m, halves=(0, 1)):
        for h in halves:
            c = place[h]
            first_copy(h, m, 0).wait_recv()
            in1[h, m, 0] = in1[h, m, 0] + part[h, m, lax.rem(c + 1, 4), 0]
            first_copy(h, m, 4).start()
            first_copy(h, m, 2).wait_recv()
            in1[h, m, 2] = in1[h, m, 2] + part[h, m, lax.rem(c + 3, 4), 1]
            first_copy(h, m, 5).start()

    def stage3(m, halves=(0, 1)):
        for h in halves:
            c = place[h]
            for k in (1, 3, 4, 5):
                first_copy(h, m, k).wait_recv()
            mid[h, m, :, 0] = part[h, m, c, 0] + in1[h, m, 3] + in1[h, m, 4]
            mid[h, m, :, 1] = part[h, m, c, 1] + in1[h, m, 1] + in1[h, m, 5]
            for k in (0, 2, 1, 3):
                second_copy(h, m, k).start()

    def stage4(m, halves=(0, 1)):
        for h in halves:
            c = place[1 - h]
            second_copy(h, m, 0).wait_recv()
            in2[h, m, 0] = in2[h, m, 0] + mid[h, m, lax.rem(c + 1, 4), 0]
            second_copy(h, m, 4).start()
            second_copy(h, m, 2).wait_recv()
            in2[h, m, 2] = in2[h, m, 2] + mid[h, m, lax.rem(c + 3, 4), 1]
            second_copy(h, m, 5).start()

    def second_sum(h, m):
        c = place[1 - h]
        for k in (1, 3, 4, 5):
            second_copy(h, m, k).wait_recv()
        low[h, m, 0] = mid[h, m, c, 0] + in2[h, m, 3] + in2[h, m, 4]
        low[h, m, 1] = mid[h, m, c, 1] + in2[h, m, 1] + in2[h, m, 5]

    def stage5(m):
        for h in range(2):
            second_sum(h, m)
            z_copy(h, m).start()


    def aux_parts():
        def line(m, carry):
            out = jnp.dot(xt[...], q[m], preferred_element_type=f32)
            for j in range(4):
                for k in range(3):
                    part[1, aux, m // 2, lax.rem(m, 2), j, 8 + 8 * k : 16 + 8 * k] = out[
                        8 * j : 8 * j + 8, 128 * k : 128 * k + 128
                    ]
            return carry

        lax.fori_loop(0, mats, line, 0)
        ends = jnp.dot(xt[32:48, :], q[0], preferred_element_type=f32)[:8]
        squares = q[0, :, :256].astype(f32)
        squares = jnp.sum(squares * squares, axis=0, keepdims=True)
        second = iota((8, 128), 0) == 1
        for k in range(3):
            piece = ends[:, 128 * k : 128 * k + 128]
            if k < 2:
                piece = jnp.where(second, squares[:, 128 * k : 128 * k + 128], piece)
            part[1, aux, 3, 1, 0, 8 + 8 * k : 16 + 8 * k] = piece
        for j in range(1, 4):
            part[1, aux, 3, 1, j, 8:32] = jnp.zeros((24, 128), f32)
        group = iota((rows, 128), 1) // 32
        last = jnp.where(
            core == 0,
            q[3, :, 256:].astype(f32),
            jnp.where(iota((rows, 128), 1) == 96, 1.0, 0.0),
        )
        picked = last
        for k in range(3):
            picked = jnp.where(group == k, q[4 * core + k, :, 256:].astype(f32), picked)
        picked = picked.astype(bf16)
        square_at = (iota((256, 128), 1) == 97) & (core == 1)

        def block(yb, carry):
            lines = yt[pl.ds(pl.multiple_of(yb * 256, 256), 256), :]
            out = jnp.dot(lines, picked, preferred_element_type=f32)
            wide = lines.astype(f32)
            out = jnp.where(square_at, jnp.sum(wide * wide, axis=1, keepdims=True), out)
            tps[pl.ds(pl.multiple_of(yb * 8, 8), 8)] = out.reshape(8, 32, 128)
            return carry

        lax.fori_loop(0, 4, block, 0)
        mine = tps[:, pl.ds(pl.multiple_of(zl * 8, 8), 8), :]
        part[1, aux, :, :, :, 0:8] = mine.reshape(4, 2, 4, 8, 128)

    def both_copy():
        return remote(low.at[1, aux], lowin, sendx.at[0], recvx.at[0], z_peer)

    def along_y(d):
        return remote(
            agu.at[x, y], agu.at[x, y], sendx.at[d], recvx.at[d], at_y(y + d)
        )

    def along_x(k):
        if k < 2:
            ref = agu.at[x]
        elif k == 2:
            ref = agu.at[lax.rem(x + 3, 4), pl.ds(0, 2)]
        else:
            ref = agu.at[lax.rem(x + 1, 4), pl.ds(2, 2)]
        return remote(ref, ref, sendx.at[4 + k], recvx.at[4 + k], peers[0][k % 2])

    def aux_low():
        second_sum(1, aux)
        both_copy().start()

    def aux_total():
        both_copy().wait_recv()
        total = low[1, aux] + lowin[...]
        agu[x, y] = total[:, 8:]
        for d in range(1, 4):
            along_y(d).start()
        tt[t] = jnp.where(zh == 0, total[0, :8], total[1, :8])
        for d in range(1, 8):
            to_tile(tt.at[t], tt.at[t], 0, d).start()

    def aux_row():
        for d in range(1, 4):
            along_y(d).wait_recv()
        along_x(0).start()
        along_x(1).start()

    def aux_pass():
        along_x(0).wait_recv()
        along_x(1).wait_recv()
        along_x(2).start()
        along_x(3).start()

    def solve():
        along_x(2).wait_recv()
        along_x(3).wait_recv()
        for d in range(1, 8):
            to_tile(tt.at[t], tt.at[t], 0, d).wait_recv()
        lane = iota((32, 128), 1)
        row = iota((32, 128), 0)
        lane8 = iota((8, 128), 1)
        row8 = iota((8, 128), 0)

        def eight(k):
            return agu[0, 3, 1, 8 * k : 8 * k + 8]

        def product(m, k):
            return agu[:, m // 2, m % 2, 8 * k : 8 * k + 8].reshape(32, 128)

        sums = eight(2)[0:1]
        sum_column = jnp.sum(jnp.where(lane == row, sums, 0.0), axis=1, keepdims=True)
        sum_rows = jnp.where(
            row8 == 0, jnp.where(lane8 < 32, sums, jnp.where(lane8 == 32, samples, 0.0)), 0.0
        )
        ones_g = jnp.concatenate([eight(0), eight(1)], axis=1)
        ones_rows = jnp.where(iota((8, 256), 0) == 0, ones_g, 0.0)

        def gram_of(m):
            body = jnp.where(lane < 32, product(m, 2), jnp.where(lane == 32, sum_column, 0.0))
            return jnp.concatenate([body, sum_rows], axis=0)

        def geno_of(m):
            body = jnp.concatenate([product(m, 0), product(m, 1)], axis=1)
            return jnp.concatenate([body, ones_rows], axis=0)

        trait_sums = [
            jnp.concatenate([tt[2 * k + c] for k in range(4)], axis=0) for c in range(2)
        ]
        ones_y = trait_sums[1][:, 96:97]
        squares_y = trait_sums[1][:, 97:98]

        def trait_of(m):
            own = trait_sums[m // 4]
            k = m % 4
            if k:
                own = pltpu.roll(own, 128 - 32 * k, 1)
            return jnp.where(lane < 32, own, jnp.where(lane == 32, ones_y, 0.0))

        gram = gram_of(0)
        inv = gram
        lane40 = iota((40, 128), 1)
        row40 = iota((40, 128), 0)
        for k in range(C + 1):
            pivot = inv[k : k + 1, k : k + 1]
            line = jnp.where(lane8[:1] == k, 1.0, inv[k : k + 1, :]) / pivot
            column = inv[:, k : k + 1]
            rest = jnp.where(lane40 == k, 0.0, inv)
            inv = jnp.where(row40 == k, line, rest - column * line)
        pad128 = jnp.zeros((88, 128), f32)
        pad256 = jnp.zeros((88, 256), f32)
        geno0 = geno_of(0)
        coef_g = exact_dot(inv, jnp.concatenate([geno0, pad256], axis=0))
        coef_g = coef_g.astype(bf16).astype(f32)
        trait0 = trait_of(0)
        coef_t = exact_dot(trait0, jnp.concatenate([inv, pad128], axis=0))
        coef_t = coef_t.astype(bf16).astype(f32)
        for m in range(mats):
            lhs[m * 40 : m * 40 + 40] = gram_of(m)
            lhs[mats * 40 + m * 32 : mats * 40 + m * 32 + 32] = trait_of(m)
        out = exact_dot(lhs[...], jnp.concatenate([coef_g, pad256], axis=0))
        for m in range(mats):
            left = geno_of(m) - out[m * 40 : m * 40 + 40]
            vst[:40, m * 256 : m * 256 + 256] = left
            vst[40:, m * 256 : m * 256 + 256] = pad256
            if m == 0:
                squares_g = ones_g[1:2] - jnp.sum(
                    coef_g * (geno0 + left), axis=0, keepdims=True
                )
        more = exact_dot(coef_t, vst[...])
        for m in range(mats):
            at = mats * 40 + m * 32
            corr[m] = out[at : at + 32] + more[:, m * 256 : m * 256 + 256]
        back = exact_dot(coef_t, jnp.concatenate([gram, pad128], axis=0))
        squares_t = squares_y - jnp.sum(coef_t * (2.0 * trait0 - back), axis=1, keepdims=True)
        mean_t = jnp.maximum(squares_t, 0.0) / samples
        mean_g = jnp.maximum(squares_g, 0.0) / samples
        factor_z = math.sqrt(samples - C - 2) / samples
        st_ref[...] = jnp.broadcast_to(lax.rsqrt(mean_t + epsilon) * factor_z, (32, 128))
        sg_ref[...] = jnp.broadcast_to(lax.rsqrt(mean_g + epsilon), (8, 256))

    def owned(m):
        outs = []
        for h in range(2):
            z_copy(h, m).wait_recv()
            cols = slice(h * 128, h * 128 + 128)
            total = low[h, m, zh] + inz[h, m] - corr[m, :, cols]
            outs.append(total * st_ref[...] * sg_ref[0:1, cols])
        return outs

    spread = jnp.where(lax.rem(iota((32, 128), 1), 32) == iota((32, 128), 0), 1.0, 0.0)
    spread = spread.astype(bf16)
    for b in range(4):
        at = slice(b * 256, b * 256 + 256)
        q[0, at, :256] = geno_ref[at, :].astype(f32).astype(bf16)
        q[0, at, 256:] = jnp.dot(
            cov_ref[at, :], spread, preferred_element_type=f32
        ).astype(bf16)
    pick = jnp.where(iota((48, 32), 0) == iota((48, 32), 1), 1.0, 0.0).astype(bf16)
    lines = across(pick, cov_ref[...])
    xt[...] = jnp.where(iota((48, rows), 0) == 32, 1.0, lines).astype(bf16)
    eye = jnp.where(iota((256, 256), 0) == iota((256, 256), 1), 1.0, 0.0).astype(bf16)

    def flip(b, carry):
        at = pl.ds(pl.multiple_of(b * 256, 256), 256)
        yt[at, :] = across(eye, y_ref[:, at]).astype(bf16)
        return carry

    lax.fori_loop(0, 4, flip, 0)

    def early(m, carry):
        @pl.when(m >= 1)
        def _():
            permute(m)

        @pl.when(m < 2)
        def _():
            compute(m)

        @pl.when(m == 0)
        def _():
            pl.semaphore_wait(barrier, 13)

        @pl.when(m < 2)
        def _():
            stage1(m)

        return carry

    lax.fori_loop(0, mats, early, 0)
    aux_parts()
    stage1(aux, (1,))
    stage2(0)

    first_step = 2
    steps = {
        2: (lambda: stage2(aux, (1,)), lambda: stage3(aux, (1,))),
        3: (lambda: stage4(aux, (1,)), aux_low),
        4: (aux_total, aux_row),
        5: (aux_pass, solve),
    }

    def step(i, carry):
        def small(part_of):
            for at, pair in steps.items():
                @pl.when(i == at)
                def _(pair=pair):
                    pair[part_of]()

        small(0)

        @pl.when(i < mats)
        def _():
            compute(i)
            stage1(i)

        @pl.when(i < mats + 1)
        def _():
            stage2(i - 1)

        small(1)

        for lag, stage in ((2, stage3), (3, stage4), (4, stage5)):
            @pl.when((i >= lag) & (i < mats + lag))
            def _(stage=stage, lag=lag):
                stage(i - lag)

        return carry

    lax.fori_loop(first_step, mats + 4, step, 0)

    left, right = owned(0)
    obs_ref[:, :128] = left
    obs_ref[:, 128:] = right
    lane = iota((32, 128), 1)
    best = jnp.zeros((32, 128), f32)
    for m in range(1, mats):
        left, right = owned(m)
        peak = jnp.max(jnp.maximum(jnp.abs(left), jnp.abs(right)), axis=1, keepdims=True)
        best = jnp.where(lane == m - 1, peak, best)
    pm[...] = best
    for d in range(1, 8):
        to_tile(pm, pmin.at[d - 1], 1, d).start()

    def drain(m, carry):
        for h in range(2):
            for k in range(6):
                first_copy(h, m, k).wait_send()
                second_copy(h, m, k).wait_send()
            z_copy(h, m).wait_send()
        return carry

    lax.fori_loop(0, mats, drain, 0)
    for k in range(6):
        first_copy(1, aux, k).wait_send()
        second_copy(1, aux, k).wait_send()
    both_copy().wait_send()
    for d in range(1, 4):
        along_y(d).wait_send()
    for k in range(4):
        along_x(k).wait_send()
    for d in range(1, 8):
        to_tile(tt.at[t], tt.at[t], 0, d).wait_send()
    for d in range(1, 8):
        to_tile(pm, pmin.at[d - 1], 1, d).wait_recv()
        best = jnp.maximum(best, pmin[d - 1])
    peak_ref[...] = best
    for d in range(1, 8):
        to_tile(pm, pmin.at[d - 1], 1, d).wait_send()


def scan(traits, covariates, genotypes, shuffles, samples):
    perms = shuffles.shape[0]
    mats = perms + 1
    rows = traits.shape[0]
    vmem = pl.BlockSpec(memory_space=pltpu.VMEM)
    dma = pltpu.SemaphoreType.DMA
    return pl.pallas_call(
        functools.partial(scan_kernel, samples=samples),
        out_shape=(
            jax.ShapeDtypeStruct((32, 256), f32),
            jax.ShapeDtypeStruct((32, 128), f32),
        ),
        in_specs=[vmem] * 4,
        out_specs=(vmem, vmem),
        scratch_shapes=[
            pltpu.VMEM((1024, rows), bf16),
            pltpu.VMEM((mats, rows, 384), bf16),
            pltpu.VMEM((48, rows), bf16),
            pltpu.VMEM((32, 32, 128), f32),
            pltpu.VMEM((2, mats + 1, 4, 2, 4, 32, 128), f32),
            pltpu.VMEM((2, mats + 1, 6, 4, 32, 128), f32),
            pltpu.VMEM((2, mats + 1, 4, 2, 32, 128), f32),
            pltpu.VMEM((2, mats + 1, 6, 32, 128), f32),
            pltpu.VMEM((2, mats + 1, 2, 32, 128), f32),
            pltpu.VMEM((2, mats, 32, 128), f32),
            pltpu.VMEM((2, 32, 128), f32),
            pltpu.VMEM((4, 4, 2, 24, 128), f32),
            pltpu.VMEM((8, 8, 128), f32),
            pltpu.VMEM((mats * 72, 128), f32),
            pltpu.VMEM((128, mats * 256), f32),
            pltpu.VMEM((mats, 32, 256), f32),
            pltpu.VMEM((32, 128), f32),
            pltpu.VMEM((8, 256), f32),
            pltpu.VMEM((32, 128), f32),
            pltpu.VMEM((7, 32, 128), f32),
            dma((2, mats + 1, 6)), dma((2, mats + 1, 6)),
            dma((2, mats + 1, 6)), dma((2, mats + 1, 6)),
            dma((2, mats)), dma((2, mats)),
            dma((8,)), dma((8,)),
            dma((2, 7)), dma((2, 7)),
        ],
        compiler_params=pltpu.CompilerParams(
            collective_id=0, has_side_effects=True, vmem_limit_bytes=56 * 1024 * 1024
        ),
    )(traits, covariates, genotypes, shuffles)


def shards(traits, covariates, genotypes, shuffles):
    samples = traits.shape[0] * lax.axis_size("samp")
    observed, peaks = scan(traits, covariates, genotypes, shuffles, samples)
    return (observed, peaks[:, : shuffles.shape[0]].T)


def solution(mesh):
    placed = (P("samp", None), P("samp", None), P("samp", "tile"), P(None, "samp"))
    return jax.shard_map(
        shards,
        mesh=mesh,
        in_specs=placed,
        out_specs=(P("samp", "tile"), P(None, "samp")),
        check_vma=False,
    )
```

```python
import functools
import math

import jax
import jax.numpy as jnp
from jax import lax
from jax.experimental import pallas as pl
from jax.experimental.pallas import tpu as pltpu
from jax.sharding import PartitionSpec as P

C = 32


epsilon = 1e-05
MESH = pl.DeviceIdType.MESH
f32 = jnp.float32
bf16 = jnp.bfloat16


def exact_dot(a, b):
    return jnp.dot(a, b, preferred_element_type=f32, precision=lax.Precision.HIGHEST)


def across(a, b):
    return lax.dot_general(a, b, (((1,), (1,)), ((), ())), preferred_element_type=f32)


def iota(shape, dim):
    return lax.broadcasted_iota(jnp.int32, shape, dim)


def scan_kernel(
    y_ref, cov_ref, geno_ref, order_ref, obs_ref, peak_ref,
    yt, q, xt, tps, part, in1, mid, in2, low, inz, ind, agu, tt,
    lhs, vst, corr, st_ref, sg_ref, pm, pmin,
    send1, recv1, send2, recv2, sendz, recvz, sendd, recvd, sendx, recvx,
    *, samples,
):
    perms = order_ref.shape[0]
    mats = perms + 1
    own = perms
    aux = mats
    ringed = perms - 1
    rows = y_ref.shape[0]
    s = lax.axis_index("samp")
    t = lax.axis_index("tile")
    x = lax.rem(s, 4)
    zh = lax.rem(s // 4, 2)
    y = s // 8
    core = lax.rem(t, 2)
    zl = t // 2
    base = s * rows

    def at_x(d, dz=0):
        return y * 8 + lax.rem(zh + dz, 2) * 4 + lax.rem(x + d, 4)

    def at_y(d, dz=0):
        return lax.rem(y + d, 4) * 8 + lax.rem(zh + dz, 2) * 4 + x

    place = (x, y)
    along = (at_x, at_y)
    apart = [(d, dz) for d in range(4) for dz in range(2) if d or dz]

    barrier = pltpu.get_barrier_semaphore()
    met = [at_y(d, dz) for d, dz in apart] + [at_x(d, dz) for d, dz in apart if d]
    for peer in met:
        pl.semaphore_signal(barrier, inc=1, device_id={"samp": peer}, device_id_type=MESH)
    for d in range(1, 8):
        pl.semaphore_signal(
            barrier, inc=1, device_id={"tile": lax.rem(t + d, 8)}, device_id_type=MESH
        )

    def remote(src, dst, send, recv, peer):
        return pltpu.make_async_remote_copy(
            src_ref=src, dst_ref=dst, send_sem=send, recv_sem=recv,
            device_id={"samp": peer}, device_id_type=MESH,
        )

    def to_tile(src, dst, k, d):
        return pltpu.make_async_remote_copy(
            src_ref=src, dst_ref=dst, send_sem=sendx.at[k], recv_sem=recvx.at[k],
            device_id={"tile": lax.rem(t + d, 8)}, device_id_type=MESH,
        )

    def all_of(ref, send, recv):
        return remote(ref, ref, send, recv, at_x(1))

    def ring_copy(src, buf, h, m, k, c, peers, send, recv):
        blk = lax.rem(c + (2, 2, 1, 3, 1, 3)[k], 4)
        uv = (0, 1, 1, 0, 0, 1)[k]
        ref = buf.at[h, m, k - 4] if k >= 4 else src.at[h, m, blk, uv]
        return remote(
            ref, buf.at[h, m, k], send.at[h], recv.at[h, m, min(k, 2)],
            peers((1, 3, 1, 3, 1, 3)[k]),
        )

    def first_copy(h, m, k):
        return ring_copy(part, in1, h, m, k, place[h], along[h], send1, recv1)

    def second_copy(h, m, k):
        return ring_copy(mid, in2, h, m, k, place[1 - h], along[1 - h], send2, recv2)

    def z_copy(h, m):
        return remote(
            low.at[h, m, 1 - zh], inz.at[h, m], sendz.at[h], recvz.at[h, m], at_x(0, 1)
        )

    def compute(m):
        def block(yb, carry):
            lines = yt[pl.ds(pl.multiple_of(yb * 256, 256), 256), :]
            out = jnp.dot(lines, q[m, :, :256], preferred_element_type=f32)
            for z in range(2):
                for xb in range(4):
                    at = (z * 4 + xb) * 32
                    part[0, m, xb, z, yb] = out[at : at + 32, :128]
                    part[1, m, yb, z, xb] = out[at : at + 32, 128:]
            return carry

        lax.fori_loop(0, 4, block, 0)

    def permute(m):
        order = order_ref[pl.ds(m, 1), :] - base

        def block(jb, carry):
            target = iota((256, rows), 0) + jb * 256
            hot = jnp.where(target == order, 1.0, 0.0).astype(bf16)
            moved = jnp.dot(hot, q[own], preferred_element_type=f32)
            q[m, pl.ds(pl.multiple_of(jb * 256, 256), 256), :] = moved.astype(bf16)
            return carry

        lax.fori_loop(0, 4, block, 0)

    def stage1(m, halves=(0, 1)):
        for k in range(4):
            for h in halves:
                first_copy(h, m, k).start()

    def stage2(m, halves=(0, 1)):
        for h in halves:
            c = place[h]
            for k, d, uv in ((0, 1, 0), (1, 3, 1)):
                first_copy(h, m, k).wait_recv()
                in1[h, m, k] = in1[h, m, k] + part[h, m, lax.rem(c + d, 4), uv]
                first_copy(h, m, k + 4).start()

    def first_sum(h, m):
        c = place[h]
        all_of(in1.at[h, m, pl.ds(2, 4)], send1.at[h], recv1.at[h, m, 2]).wait_recv()
        mid[h, m, :, 0] = part[h, m, c, 0] + in1[h, m, 3] + in1[h, m, 4]
        mid[h, m, :, 1] = part[h, m, c, 1] + in1[h, m, 2] + in1[h, m, 5]

    def stage3(m):
        for h in range(2):
            first_sum(h, m)
            for k in range(4):
                second_copy(h, m, k).start()

    def stage4(m):
        for h in range(2):
            c = place[1 - h]
            for k, d, uv in ((0, 1, 0), (1, 3, 1)):
                second_copy(h, m, k).wait_recv()
                in2[h, m, k] = in2[h, m, k] + mid[h, m, lax.rem(c + d, 4), uv]
                second_copy(h, m, k + 4).start()

    def stage5(m):
        for h in range(2):
            c = place[1 - h]
            all_of(in2.at[h, m, pl.ds(2, 4)], send2.at[h], recv2.at[h, m, 2]).wait_recv()
            low[h, m, 0] = mid[h, m, c, 0] + in2[h, m, 3] + in2[h, m, 4]
            low[h, m, 1] = mid[h, m, c, 1] + in2[h, m, 2] + in2[h, m, 5]
            z_copy(h, m).start()


    def direct(m, halves=(0, 1)):
        for h in halves:
            first_sum(h, m)
            for k, (d, dz) in enumerate(apart):
                blk = lax.rem(place[1 - h] + d, 4)
                remote(
                    mid.at[h, m, blk, lax.rem(zh + dz, 2)], ind.at[h, m - ringed, k],
                    sendd.at[h], recvd.at[h, m - ringed], along[1 - h](d, dz),
                ).start()

    def direct_sum(h, m):
        n = m - ringed
        all_of(ind.at[h, n], sendd.at[h], recvd.at[h, n]).wait_recv()
        total = mid[h, m, place[1 - h], zh]
        for k in range(7):
            total = total + ind[h, n, k]
        return total


    def aux_parts():
        def line(m, carry):
            out = jnp.dot(xt[...], q[m], preferred_element_type=f32)
            for j in range(4):
                for k in range(3):
                    part[1, aux, m // 2, lax.rem(m, 2), j, 8 + 8 * k : 16 + 8 * k] = out[
                        8 * j : 8 * j + 8, 128 * k : 128 * k + 128
                    ]
            return carry

        lax.fori_loop(0, mats, line, 0)
        ends = jnp.dot(xt[32:48, :], q[own], preferred_element_type=f32)[:8]
        squares = q[own, :, :256].astype(f32)
        squares = jnp.sum(squares * squares, axis=0, keepdims=True)
        second = iota((8, 128), 0) == 1
        for k in range(3):
            piece = ends[:, 128 * k : 128 * k + 128]
            if k < 2:
                piece = jnp.where(second, squares[:, 128 * k : 128 * k + 128], piece)
            part[1, aux, 3, 1, 0, 8 + 8 * k : 16 + 8 * k] = piece
        for j in range(1, 4):
            part[1, aux, 3, 1, j, 8:32] = jnp.zeros((24, 128), f32)
        group = iota((rows, 128), 1) // 32
        last = jnp.where(
            core == 0,
            q[3, :, 256:].astype(f32),
            jnp.where(iota((rows, 128), 1) == 96, 1.0, 0.0),
        )
        picked = last
        for k in range(3):
            picked = jnp.where(group == k, q[4 * core + k, :, 256:].astype(f32), picked)
        picked = picked.astype(bf16)
        square_at = (iota((256, 128), 1) == 97) & (core == 1)

        def block(yb, carry):
            lines = yt[pl.ds(pl.multiple_of(yb * 256, 256), 256), :]
            out = jnp.dot(lines, picked, preferred_element_type=f32)
            wide = lines.astype(f32)
            out = jnp.where(square_at, jnp.sum(wide * wide, axis=1, keepdims=True), out)
            tps[pl.ds(pl.multiple_of(yb * 8, 8), 8)] = out.reshape(8, 32, 128)
            return carry

        lax.fori_loop(0, 4, block, 0)
        mine = tps[:, pl.ds(pl.multiple_of(zl * 8, 8), 8), :]
        part[1, aux, :, :, :, 0:8] = mine.reshape(4, 2, 4, 8, 128)

    def aux_total():
        total = direct_sum(1, aux)
        agu[x, y * 2 + zh] = total[8:]
        tt[t] = total[:8]
        for d, dz in apart:
            ref = agu.at[x, y * 2 + zh]
            remote(ref, ref, sendx.at[2], recvx.at[2], at_y(d, dz)).start()
        for d in range(1, 8):
            to_tile(tt.at[t], tt.at[t], 0, d).start()

    def aux_row():
        all_of(agu.at[x, pl.ds(0, 7)], sendx.at[2], recvx.at[2]).wait_recv()
        for d in (1, 3, 2):
            remote(agu.at[x], agu.at[x], sendx.at[3], recvx.at[3], at_x(d)).start()

    def solve():
        all_of(agu.at[pl.ds(0, 3)], sendx.at[3], recvx.at[3]).wait_recv()
        all_of(tt.at[pl.ds(0, 7)], sendx.at[0], recvx.at[0]).wait_recv()
        lane = iota((32, 128), 1)
        row = iota((32, 128), 0)
        lane8 = iota((8, 128), 1)
        row8 = iota((8, 128), 0)

        def eight(k):
            return agu[0, 7, 8 * k : 8 * k + 8]

        def product(m, k):
            return agu[:, m, 8 * k : 8 * k + 8].reshape(32, 128)

        sums = eight(2)[0:1]
        sum_column = jnp.sum(jnp.where(lane == row, sums, 0.0), axis=1, keepdims=True)
        sum_rows = jnp.where(
            row8 == 0, jnp.where(lane8 < 32, sums, jnp.where(lane8 == 32, samples, 0.0)), 0.0
        )
        ones_g = jnp.concatenate([eight(0), eight(1)], axis=1)
        ones_rows = jnp.where(iota((8, 256), 0) == 0, ones_g, 0.0)

        def gram_of(m):
            body = jnp.where(lane < 32, product(m, 2), jnp.where(lane == 32, sum_column, 0.0))
            return jnp.concatenate([body, sum_rows], axis=0)

        def geno_of(m):
            body = jnp.concatenate([product(m, 0), product(m, 1)], axis=1)
            return jnp.concatenate([body, ones_rows], axis=0)

        trait_sums = [
            jnp.concatenate([tt[2 * k + c] for k in range(4)], axis=0) for c in range(2)
        ]
        ones_y = trait_sums[1][:, 96:97]
        squares_y = trait_sums[1][:, 97:98]

        def trait_of(m):
            mine = trait_sums[m // 4]
            k = m % 4
            if k:
                mine = pltpu.roll(mine, 128 - 32 * k, 1)
            return jnp.where(lane < 32, mine, jnp.where(lane == 32, ones_y, 0.0))

        gram = gram_of(own)
        inv = gram
        lane40 = iota((40, 128), 1)
        row40 = iota((40, 128), 0)
        for k in range(C + 1):
            pivot = inv[k : k + 1, k : k + 1]
            line = jnp.where(lane8[:1] == k, 1.0, inv[k : k + 1, :]) / pivot
            column = inv[:, k : k + 1]
            rest = jnp.where(lane40 == k, 0.0, inv)
            inv = jnp.where(row40 == k, line, rest - column * line)
        pad128 = jnp.zeros((88, 128), f32)
        pad256 = jnp.zeros((88, 256), f32)
        geno0 = geno_of(own)
        coef_g = exact_dot(inv, jnp.concatenate([geno0, pad256], axis=0))
        coef_g = coef_g.astype(bf16).astype(f32)
        trait0 = trait_of(own)
        coef_t = exact_dot(trait0, jnp.concatenate([inv, pad128], axis=0))
        coef_t = coef_t.astype(bf16).astype(f32)
        for m in range(mats):
            lhs[m * 40 : m * 40 + 40] = gram_of(m)
            lhs[mats * 40 + m * 32 : mats * 40 + m * 32 + 32] = trait_of(m)
        out = exact_dot(lhs[...], jnp.concatenate([coef_g, pad256], axis=0))
        for m in range(mats):
            left = geno_of(m) - out[m * 40 : m * 40 + 40]
            vst[:40, m * 256 : m * 256 + 256] = left
            vst[40:, m * 256 : m * 256 + 256] = pad256
            if m == own:
                squares_g = ones_g[1:2] - jnp.sum(
                    coef_g * (geno0 + left), axis=0, keepdims=True
                )
        more = exact_dot(coef_t, vst[...])
        for m in range(mats):
            at = mats * 40 + m * 32
            corr[m] = out[at : at + 32] + more[:, m * 256 : m * 256 + 256]
        back = exact_dot(coef_t, jnp.concatenate([gram, pad128], axis=0))
        squares_t = squares_y - jnp.sum(coef_t * (2.0 * trait0 - back), axis=1, keepdims=True)
        mean_t = jnp.maximum(squares_t, 0.0) / samples
        mean_g = jnp.maximum(squares_g, 0.0) / samples
        factor_z = math.sqrt(samples - C - 2) / samples
        st_ref[...] = jnp.broadcast_to(lax.rsqrt(mean_t + epsilon) * factor_z, (32, 128))
        sg_ref[...] = jnp.broadcast_to(lax.rsqrt(mean_g + epsilon), (8, 256))

    def owned(m):
        outs = []
        for h in range(2):
            if m < ringed:
                z_copy(h, m).wait_recv()
                total = low[h, m, zh] + inz[h, m]
            else:
                total = direct_sum(h, m)
            cols = slice(h * 128, h * 128 + 128)
            outs.append((total - corr[m, :, cols]) * st_ref[...] * sg_ref[0:1, cols])
        return outs

    spread = jnp.where(lax.rem(iota((32, 128), 1), 32) == iota((32, 128), 0), 1.0, 0.0)
    spread = spread.astype(bf16)
    for b in range(4):
        at = slice(b * 256, b * 256 + 256)
        q[own, at, :256] = geno_ref[at, :].astype(f32).astype(bf16)
        q[own, at, 256:] = lax.dot_general(
            cov_ref[:, at], spread, (((0,), (0,)), ((), ())), preferred_element_type=f32
        ).astype(bf16)
    xt[:32] = cov_ref[...]
    xt[32:] = jnp.where(iota((16, rows), 0) == 0, 1.0, 0.0).astype(bf16)
    eye = jnp.where(iota((256, 256), 0) == iota((256, 256), 1), 1.0, 0.0).astype(bf16)

    def flip(b, carry):
        at = pl.ds(pl.multiple_of(b * 256, 256), 256)
        yt[at, :] = across(eye, y_ref[:, at]).astype(bf16)
        return carry

    lax.fori_loop(0, 4, flip, 0)
    last = mats + 1

    def step(i, carry):
        @pl.when(i < 1)
        def _():
            permute(0)

        @pl.when(i < mats)
        def _():
            compute(i)

        @pl.when(i == 0)
        def _():
            pl.semaphore_wait(barrier, len(met) + 7)

        @pl.when(i < mats)
        def _():
            stage1(i)

        @pl.when((i >= 1) & (i < mats + 1))
        def _():
            stage2(i - 1)

        @pl.when(i == 0)
        def _():
            permute(1)

        @pl.when((i >= 1) & (i < 3))
        def _():
            permute(2 * i)
            permute(2 * i + 1)

        def small(*pairs):
            for at, work in pairs:
                @pl.when(i == at)
                def _(work=work):
                    work()

        def aux_start():
            aux_parts()
            stage1(aux, (1,))

        small((3, aux_start), (4, lambda: stage2(aux, (1,))), (5, aux_total), (6, aux_row))

        @pl.when((i >= 2) & (i < ringed + 2))
        def _():
            stage3(i - 2)

        @pl.when((i >= ringed + 2) & (i < mats + 2))
        def _():
            direct(i - 2)

        small((4, lambda: direct(aux, (1,))), (7, solve))

        @pl.when((i >= 3) & (i < ringed + 3))
        def _():
            stage4(i - 3)

        @pl.when((i >= 4) & (i < ringed + 4))
        def _():
            stage5(i - 4)

        return carry

    lax.fori_loop(0, mats + 2, step, 0)

    lane = iota((32, 128), 1)
    best = jnp.zeros((32, 128), f32)
    for m in range(perms):
        left, right = owned(m)
        peak = jnp.max(jnp.maximum(jnp.abs(left), jnp.abs(right)), axis=1, keepdims=True)
        best = jnp.where(lane == m, peak, best)
    pm[...] = best
    for d in range(1, 8):
        to_tile(pm, pmin.at[d - 1], 1, d).start()
    left, right = owned(own)
    obs_ref[:, :128] = left
    obs_ref[:, 128:] = right

    for h in range(2):
        all_of(in1.at[h, pl.ds(0, mats + h)], send1.at[h], recv1.at[0, 0, 0]).wait_send()
        all_of(in2.at[h], send2.at[h], recv2.at[0, 0, 0]).wait_send()
        all_of(inz.at[h], sendz.at[h], recvz.at[0, 0]).wait_send()
        all_of(ind.at[h, pl.ds(0, 2 + h)], sendd.at[h], recvd.at[0, 0]).wait_send()
    all_of(tt.at[pl.ds(0, 7)], sendx.at[0], recvx.at[0]).wait_send()
    all_of(agu.at[x, pl.ds(0, 7)], sendx.at[2], recvx.at[2]).wait_send()
    all_of(agu.at[pl.ds(0, 3)], sendx.at[3], recvx.at[3]).wait_send()
    all_of(pmin, sendx.at[1], recvx.at[1]).wait()
    for d in range(7):
        best = jnp.maximum(best, pmin[d])
    peak_ref[...] = best


def scan(traits, covariates, genotypes, shuffles, samples):
    perms = shuffles.shape[0]
    mats = perms + 1
    rows = traits.shape[0]
    vmem = pl.BlockSpec(memory_space=pltpu.VMEM)
    dma = pltpu.SemaphoreType.DMA
    return pl.pallas_call(
        functools.partial(scan_kernel, samples=samples),
        out_shape=(
            jax.ShapeDtypeStruct((32, 256), f32),
            jax.ShapeDtypeStruct((32, 128), f32),
        ),
        in_specs=[vmem] * 4,
        out_specs=(vmem, vmem),
        scratch_shapes=[
            pltpu.VMEM((1024, rows), bf16),
            pltpu.VMEM((mats, rows, 384), bf16),
            pltpu.VMEM((48, rows), bf16),
            pltpu.VMEM((32, 32, 128), f32),
            pltpu.VMEM((2, mats + 1, 4, 2, 4, 32, 128), f32),
            pltpu.VMEM((2, mats + 1, 6, 4, 32, 128), f32),
            pltpu.VMEM((2, mats + 1, 4, 2, 32, 128), f32),
            pltpu.VMEM((2, mats - 2, 6, 32, 128), f32),
            pltpu.VMEM((2, mats - 2, 2, 32, 128), f32),
            pltpu.VMEM((2, mats - 2, 32, 128), f32),
            pltpu.VMEM((2, 3, 7, 32, 128), f32),
            pltpu.VMEM((4, 8, 24, 128), f32),
            pltpu.VMEM((8, 8, 128), f32),
            pltpu.VMEM((mats * 72, 128), f32),
            pltpu.VMEM((128, mats * 256), f32),
            pltpu.VMEM((mats, 32, 256), f32),
            pltpu.VMEM((32, 128), f32),
            pltpu.VMEM((8, 256), f32),
            pltpu.VMEM((32, 128), f32),
            pltpu.VMEM((7, 32, 128), f32),
            dma((2,)), dma((2, mats + 1, 3)),
            dma((2,)), dma((2, mats - 2, 3)),
            dma((2,)), dma((2, mats - 2)),
            dma((2,)), dma((2, 3)),
            dma((4,)), dma((4,)),
        ],
        compiler_params=pltpu.CompilerParams(
            collective_id=0, has_side_effects=True, vmem_limit_bytes=56 * 1024 * 1024
        ),
    )(traits, covariates.T, genotypes, shuffles)


def shards(traits, covariates, genotypes, shuffles):
    samples = traits.shape[0] * lax.axis_size("samp")
    observed, peaks = scan(traits, covariates, genotypes, shuffles, samples)
    return (observed, peaks[:, : shuffles.shape[0]].T)


def solution(mesh):
    placed = (P("samp", None), P("samp", None), P("samp", "tile"), P(None, "samp"))
    return jax.shard_map(
        shards,
        mesh=mesh,
        in_specs=placed,
        out_specs=(P("samp", "tile"), P(None, "samp")),
        check_vma=False,
    )
```

```python
import functools
import math

import jax
import jax.numpy as jnp
from jax import lax
from jax.experimental import pallas as pl
from jax.experimental.pallas import tpu as pltpu
from jax.sharding import PartitionSpec as P

C = 32


epsilon = 1e-05
MESH = pl.DeviceIdType.MESH
f32 = jnp.float32
bf16 = jnp.bfloat16


ORDER = (
    "C1", "B", "11", "P3", "C3", "13", "P0", "C0", "211", "P5", "10", "P2",
    "C2", "12", "231", "P4", "201", "200", "230", "aux", "A1", "210", "221", "220",
    "C5", "311", "C4", "301", "A2", "310", "14", "C6", "331", "A3", "15", "410",
    "321", "241", "411", "A4", "320", "251", "431", "240", "421", "250", "330", "16",
    "341", "511", "A5", "340", "420", "521", "351", "401", "430", "260", "300", "441",
    "531", "350", "440", "261", "A6", "501", "510", "400", "520", "450", "451", "541",
    "540", "d61", "d60", "500", "550", "530", "551", "inv", "e60", "e61", "corr", "f3",
    "f4", "f1", "f0", "f2", "f5", "T", "f6",
)


def exact_dot(a, b):
    return jnp.dot(a, b, preferred_element_type=f32, precision=lax.Precision.HIGHEST)


def across(a, b):
    return lax.dot_general(a, b, (((1,), (1,)), ((), ())), preferred_element_type=f32)


def iota(shape, dim):
    return lax.broadcasted_iota(jnp.int32, shape, dim)


def scan_kernel(
    y_hbm, cov_hbm, geno_hbm, order_hbm, out_ref,
    y_ref, cov_ref, geno_ref, order_ref, load,
    yt, q, xt, tps, part, in1, mid, in2, low, inz, ind, lowin, agu, tt,
    lhs, vst, corr, st_ref, sg_ref, pm, pmin,
    send1, recv1, send2, recv2, sendz, recvz, sendd, recvd, sendx, recvx,
    *, samples,
):
    perms = order_hbm.shape[0]
    mats = perms + 1
    own = perms
    aux = mats
    ringed = perms - 0
    rows = y_hbm.shape[0]
    s = lax.axis_index("samp")
    t = lax.axis_index("tile")
    x = lax.rem(s, 4)
    zh = lax.rem(s // 4, 2)
    y = s // 8
    core = lax.rem(t, 2)
    zl = t // 2
    base = s * rows

    def at_x(d):
        return s - x + lax.rem(x + d, 4)

    def at_y(d):
        return lax.rem(s + 8 * d, 32)

    z_peer = s + 4 - 8 * zh

    place = (x, y)
    along = (at_x, at_y)

    barrier = pltpu.get_barrier_semaphore()
    met = [at_y(d) for d in (1, 2, 3)] + [at_x(d) for d in (1, 2, 3)] + [z_peer]
    for peer in met:
        pl.semaphore_signal(barrier, inc=1, device_id={"samp": peer}, device_id_type=MESH)
    for d in range(1, 8):
        pl.semaphore_signal(
            barrier, inc=1, device_id={"tile": lax.rem(t + d, 8)}, device_id_type=MESH
        )

    loads = [
        pltpu.make_async_copy(a, b, load.at[k])
        for k, (a, b) in enumerate(
            [(cov_hbm, cov_ref), (geno_hbm, geno_ref), (order_hbm, order_ref)]
            + [(y_hbm.at[:, pl.ds(k, 256)], y_ref.at[:, pl.ds(k, 256)]) for k in range(0, 1024, 256)]
        )
    ]
    for copy in loads:
        copy.start()

    def remote(src, dst, send, recv, peer):
        return pltpu.make_async_remote_copy(
            src_ref=src, dst_ref=dst, send_sem=send, recv_sem=recv,
            device_id={"samp": peer}, device_id_type=MESH,
        )

    def to_tile(src, dst, k, d):
        return pltpu.make_async_remote_copy(
            src_ref=src, dst_ref=dst, send_sem=sendx.at[k], recv_sem=recvx.at[k],
            device_id={"tile": lax.rem(t + d, 8)}, device_id_type=MESH,
        )

    def all_of(ref, send, recv):
        return remote(ref, ref, send, recv, at_x(1))

    def ring_copy(src, buf, h, m, k, c, peers, send, recv):
        blk = lax.rem(c + (2, 2, 1, 3, 1, 3)[k], 4)
        uv = (0, 1, 1, 0, 0, 1)[k]
        ref = buf.at[h, m, k - 4] if k >= 4 else src.at[h, m, blk, uv]
        return remote(
            ref, buf.at[h, m, k], send.at[h], recv.at[h, m, min(k, 2)],
            peers((1, 3, 1, 3, 1, 3)[k]),
        )

    def first_copy(h, m, k):
        return ring_copy(part, in1, h, m, k, place[h], along[h], send1, recv1)

    def second_copy(h, m, k):
        return ring_copy(mid, in2, h, m, k, place[1 - h], along[1 - h], send2, recv2)

    def z_copy(h, m):
        return remote(
            low.at[h, m, 1 - zh], inz.at[h, m], sendz.at[h], recvz.at[h, m], z_peer
        )

    def compute(m):
        def block(yb, carry):
            lines = yt[pl.ds(pl.multiple_of(yb * 256, 256), 256), :]
            out = jnp.dot(lines, q[m, :, :256], preferred_element_type=f32)
            for z in range(2):
                for xb in range(4):
                    at = (z * 4 + xb) * 32
                    part[0, m, xb, z, yb] = out[at : at + 32, :128]
                    part[1, m, yb, z, xb] = out[at : at + 32, 128:]
            return carry

        lax.fori_loop(0, 4, block, 0)

    def permute(m):
        order = order_ref[pl.ds(m, 1), :] - base

        def block(jb, carry):
            target = iota((256, rows), 0) + jb * 256
            hot = jnp.where(target == order, 1.0, 0.0).astype(bf16)
            moved = jnp.dot(hot, q[own], preferred_element_type=f32)
            q[m, pl.ds(pl.multiple_of(jb * 256, 256), 256), :] = moved.astype(bf16)
            return carry

        lax.fori_loop(0, 4, block, 0)

    def stage1(m, halves=(0, 1)):
        for k in range(4):
            for h in halves:
                first_copy(h, m, k).start()

    def stage2(m, halves=(0, 1)):
        for h in halves:
            c = place[h]
            for k, d, uv in ((0, 1, 0), (1, 3, 1)):
                first_copy(h, m, k).wait_recv()
                in1[h, m, k] = in1[h, m, k] + part[h, m, lax.rem(c + d, 4), uv]
                first_copy(h, m, k + 4).start()

    def first_sum(h, m):
        c = place[h]
        all_of(in1.at[h, m, pl.ds(2, 4)], send1.at[h], recv1.at[h, m, 2]).wait_recv()
        mid[h, m, :, 0] = part[h, m, c, 0] + in1[h, m, 3] + in1[h, m, 4]
        mid[h, m, :, 1] = part[h, m, c, 1] + in1[h, m, 2] + in1[h, m, 5]

    def stage3(m, halves=(0, 1)):
        for h in halves:
            first_sum(h, m)
            for k in range(4):
                second_copy(h, m, k).start()

    def stage4(m, halves=(0, 1)):
        for h in halves:
            c = place[1 - h]
            for k, d, uv in ((0, 1, 0), (1, 3, 1)):
                second_copy(h, m, k).wait_recv()
                in2[h, m, k] = in2[h, m, k] + mid[h, m, lax.rem(c + d, 4), uv]
                second_copy(h, m, k + 4).start()

    def stage5(m, halves=(0, 1)):
        for h in halves:
            c = place[1 - h]
            all_of(in2.at[h, m, pl.ds(2, 4)], send2.at[h], recv2.at[h, m, 2]).wait_recv()
            low[h, m, 0] = mid[h, m, c, 0] + in2[h, m, 3] + in2[h, m, 4]
            low[h, m, 1] = mid[h, m, c, 1] + in2[h, m, 2] + in2[h, m, 5]
            z_copy(h, m).start()


    def direct(m, halves=(0, 1)):
        for h in halves:
            first_sum(h, m)
            for d in (1, 3, 2):
                remote(
                    mid.at[h, m, lax.rem(place[1 - h] + d, 4)], ind.at[h, m - ringed, d - 1],
                    sendd.at[h], recvd.at[h, m - ringed], along[1 - h](d),
                ).start()

    def direct_sum(h, m):
        n = m - ringed
        all_of(ind.at[h, n], sendd.at[h], recvd.at[h, n]).wait_recv()
        low[h, m] = mid[h, m, place[1 - h]] + ind[h, n, 0] + ind[h, n, 1] + ind[h, n, 2]

    def stage5d(m, halves=(0, 1)):
        for h in halves:
            direct_sum(h, m)
            z_copy(h, m).start()


    def aux_parts():
        def line(m, carry):
            out = jnp.dot(xt[...], q[m], preferred_element_type=f32)
            for j in range(4):
                for k in range(3):
                    part[1, aux, m // 2, lax.rem(m, 2), j, 8 + 8 * k : 16 + 8 * k] = out[
                        8 * j : 8 * j + 8, 128 * k : 128 * k + 128
                    ]
            return carry

        lax.fori_loop(0, mats, line, 0)
        ends = jnp.dot(xt[32:48, :], q[own], preferred_element_type=f32)[:8]
        squares = q[own, :, :256].astype(f32)
        squares = jnp.sum(squares * squares, axis=0, keepdims=True)
        second = iota((8, 128), 0) == 1
        for k in range(3):
            piece = ends[:, 128 * k : 128 * k + 128]
            if k < 2:
                piece = jnp.where(second, squares[:, 128 * k : 128 * k + 128], piece)
            part[1, aux, 3, 1, 0, 8 + 8 * k : 16 + 8 * k] = piece
        for j in range(1, 4):
            part[1, aux, 3, 1, j, 8:32] = jnp.zeros((24, 128), f32)
        group = iota((rows, 128), 1) // 32
        last = jnp.where(
            core == 0,
            q[3, :, 256:].astype(f32),
            jnp.where(iota((rows, 128), 1) == 96, 1.0, 0.0),
        )
        picked = last
        for k in range(3):
            picked = jnp.where(group == k, q[4 * core + k, :, 256:].astype(f32), picked)
        picked = picked.astype(bf16)
        square_at = (iota((256, 128), 1) == 97) & (core == 1)

        def block(yb, carry):
            lines = yt[pl.ds(pl.multiple_of(yb * 256, 256), 256), :]
            out = jnp.dot(lines, picked, preferred_element_type=f32)
            wide = lines.astype(f32)
            out = jnp.where(square_at, jnp.sum(wide * wide, axis=1, keepdims=True), out)
            tps[pl.ds(pl.multiple_of(yb * 8, 8), 8)] = out.reshape(8, 32, 128)
            return carry

        lax.fori_loop(0, 4, block, 0)
        mine = tps[:, pl.ds(pl.multiple_of(zl * 8, 8), 8), :]
        part[1, aux, :, :, :, 0:8] = mine.reshape(4, 2, 4, 8, 128)

    def both_copy():
        return remote(low.at[1, aux], lowin, sendx.at[4], recvx.at[4], z_peer)

    def aux_low():
        direct_sum(1, aux)
        both_copy().start()

    def aux_total():
        both_copy().wait_recv()
        total = low[1, aux] + lowin[...]
        agu[x, y] = total[:, 8:]
        for d in (1, 3, 2):
            remote(agu.at[x, y], agu.at[x, y], sendx.at[2], recvx.at[2], at_y(d)).start()
        tt[t] = jnp.where(zh == 0, total[0, :8], total[1, :8])
        for d in range(1, 8):
            to_tile(tt.at[t], tt.at[t], 0, d).start()

    def aux_row():
        all_of(agu.at[x, pl.ds(0, 3)], sendx.at[2], recvx.at[2]).wait_recv()
        for d in (1, 3, 2):
            remote(agu.at[x], agu.at[x], sendx.at[3], recvx.at[3], at_x(d)).start()

    def solve():
        all_of(agu.at[pl.ds(0, 3)], sendx.at[3], recvx.at[3]).wait_recv()
        all_of(tt.at[pl.ds(0, 7)], sendx.at[0], recvx.at[0]).wait_recv()
        lane = iota((32, 128), 1)
        row = iota((32, 128), 0)
        lane8 = iota((8, 128), 1)
        row8 = iota((8, 128), 0)

        def eight(k):
            return agu[0, 3, 1, 8 * k : 8 * k + 8]

        def product(m, k):
            return agu[:, m // 2, m % 2, 8 * k : 8 * k + 8].reshape(32, 128)

        sums = eight(2)[0:1]
        sum_column = jnp.sum(jnp.where(lane == row, sums, 0.0), axis=1, keepdims=True)
        sum_rows = jnp.where(
            row8 == 0, jnp.where(lane8 < 32, sums, jnp.where(lane8 == 32, samples, 0.0)), 0.0
        )
        ones_g = jnp.concatenate([eight(0), eight(1)], axis=1)
        ones_rows = jnp.where(iota((8, 256), 0) == 0, ones_g, 0.0)

        def gram_of(m):
            body = jnp.where(lane < 32, product(m, 2), jnp.where(lane == 32, sum_column, 0.0))
            return jnp.concatenate([body, sum_rows], axis=0)

        def geno_of(m):
            body = jnp.concatenate([product(m, 0), product(m, 1)], axis=1)
            return jnp.concatenate([body, ones_rows], axis=0)

        trait_sums = [
            jnp.concatenate([tt[2 * k + c] for k in range(4)], axis=0) for c in range(2)
        ]
        ones_y = trait_sums[1][:, 96:97]
        squares_y = trait_sums[1][:, 97:98]

        def trait_of(m):
            mine = trait_sums[m // 4]
            k = m % 4
            if k:
                mine = pltpu.roll(mine, 128 - 32 * k, 1)
            return jnp.where(lane < 32, mine, jnp.where(lane == 32, ones_y, 0.0))

        gram = gram_of(own)
        inv = gram
        lane40 = iota((40, 128), 1)
        row40 = iota((40, 128), 0)
        for k in range(C + 1):
            pivot = inv[k : k + 1, k : k + 1]
            line = jnp.where(lane8[:1] == k, 1.0, inv[k : k + 1, :]) / pivot
            column = inv[:, k : k + 1]
            rest = jnp.where(lane40 == k, 0.0, inv)
            inv = jnp.where(row40 == k, line, rest - column * line)
        return inv, gram, gram_of, geno_of, trait_of, ones_g, squares_y

    def corrections(inv, gram, gram_of, geno_of, trait_of, ones_g, squares_y):
        pad128 = jnp.zeros((88, 128), f32)
        pad256 = jnp.zeros((88, 256), f32)
        geno0 = geno_of(own)
        coef_g = exact_dot(inv, jnp.concatenate([geno0, pad256], axis=0))
        coef_g = coef_g.astype(bf16).astype(f32)
        trait0 = trait_of(own)
        coef_t = exact_dot(trait0, jnp.concatenate([inv, pad128], axis=0))
        coef_t = coef_t.astype(bf16).astype(f32)
        for m in range(mats):
            lhs[m * 40 : m * 40 + 40] = gram_of(m)
            lhs[mats * 40 + m * 32 : mats * 40 + m * 32 + 32] = trait_of(m)
        out = exact_dot(lhs[...], jnp.concatenate([coef_g, pad256], axis=0))
        for m in range(mats):
            left = geno_of(m) - out[m * 40 : m * 40 + 40]
            vst[:40, m * 256 : m * 256 + 256] = left
            vst[40:, m * 256 : m * 256 + 256] = pad256
            if m == own:
                squares_g = ones_g[1:2] - jnp.sum(
                    coef_g * (geno0 + left), axis=0, keepdims=True
                )
        more = exact_dot(coef_t, vst[...])
        for m in range(mats):
            at = mats * 40 + m * 32
            corr[m] = out[at : at + 32] + more[:, m * 256 : m * 256 + 256]
        back = exact_dot(coef_t, jnp.concatenate([gram, pad128], axis=0))
        squares_t = squares_y - jnp.sum(coef_t * (2.0 * trait0 - back), axis=1, keepdims=True)
        mean_t = jnp.maximum(squares_t, 0.0) / samples
        mean_g = jnp.maximum(squares_g, 0.0) / samples
        factor_z = math.sqrt(samples - C - 2) / samples
        st_ref[...] = jnp.broadcast_to(lax.rsqrt(mean_t + epsilon) * factor_z, (32, 128))
        sg_ref[...] = jnp.broadcast_to(lax.rsqrt(mean_g + epsilon), (8, 256))

    def owned(m):
        outs = []
        for h in range(2):
            z_copy(h, m).wait_recv()
            total = low[h, m, zh] + inz[h, m]
            cols = slice(h * 128, h * 128 + 128)
            outs.append((total - corr[m, :, cols]) * st_ref[...] * sg_ref[0:1, cols])
        return outs

    loads[0].wait()
    loads[1].wait()
    spread = jnp.where(lax.rem(iota((32, 128), 1), 32) == iota((32, 128), 0), 1.0, 0.0)
    spread = spread.astype(bf16)
    for b in range(4):
        at = slice(b * 256, b * 256 + 256)
        q[own, at, :256] = geno_ref[at, :].astype(f32).astype(bf16)
        q[own, at, 256:] = lax.dot_general(
            cov_ref[:, at], spread, (((0,), (0,)), ((), ())), preferred_element_type=f32
        ).astype(bf16)
    xt[:32] = cov_ref[...]
    xt[32:] = jnp.where(iota((16, rows), 0) == 0, 1.0, 0.0).astype(bf16)
    eye = jnp.where(iota((256, 256), 0) == iota((256, 256), 1), 1.0, 0.0).astype(bf16)

    loads[2].wait()
    permute(1)
    for b in range(4):
        loads[3 + b].wait()
        at = slice(b * 256, b * 256 + 256)
        yt[at, :] = across(eye, y_ref[:, at]).astype(bf16)

    lane = iota((32, 128), 1)
    held = {"best": jnp.zeros((32, 128), f32)}

    def finish(m):
        left, right = owned(m)
        if m == own:
            out_ref[:32, :128] = left
            out_ref[:32, 128:] = right
            out_ref[32:, 128:] = jnp.zeros((8, 128), f32)
            return
        peak = jnp.max(jnp.maximum(jnp.abs(left), jnp.abs(right)), axis=1, keepdims=True)
        held["best"] = jnp.where(lane == m, peak, held["best"])

    def exchange():
        pm[...] = held["best"]
        for d in range(1, 8):
            to_tile(pm, pmin.at[d - 1], 1, d).start()

    def invert():
        held["solved"] = solve()

    stages = {"2": stage2, "3": stage3, "4": stage4, "5": stage5, "d": direct, "e": stage5d}
    whole = {"P": permute, "C": compute, "1": stage1, "f": finish}
    single = {
        "aux": aux_parts,
        "A1": lambda: stage1(aux, (1,)),
        "A2": lambda: stage2(aux, (1,)),
        "A3": lambda: direct(aux, (1,)),
        "A4": aux_low,
        "A5": aux_total,
        "A6": aux_row,
        "inv": invert,
        "corr": lambda: corrections(*held["solved"]),
        "T": exchange,
        "B": lambda: pl.semaphore_wait(barrier, len(met) + 7),
    }
    for name in ORDER:
        if name in single:
            single[name]()
        elif name[0] in whole:
            whole[name[0]](int(name[1]))
        else:
            stages[name[0]](int(name[1]), (int(name[2]),))
    best = held["best"]

    for h in range(2):
        all_of(in1.at[h, pl.ds(0, mats + h)], send1.at[h], recv1.at[0, 0, 0]).wait_send()
        all_of(in2.at[h], send2.at[h], recv2.at[0, 0, 0]).wait_send()
        all_of(inz.at[h], sendz.at[h], recvz.at[0, 0]).wait_send()
        all_of(ind.at[h, pl.ds(0, mats - ringed + h)], sendd.at[h], recvd.at[0, 0]).wait_send()
    all_of(tt.at[pl.ds(0, 7)], sendx.at[0], recvx.at[0]).wait_send()
    all_of(agu.at[x, pl.ds(0, 3)], sendx.at[2], recvx.at[2]).wait_send()
    both_copy().wait_send()
    all_of(agu.at[pl.ds(0, 3)], sendx.at[3], recvx.at[3]).wait_send()
    all_of(pmin, sendx.at[1], recvx.at[1]).wait()
    for d in range(7):
        best = jnp.maximum(best, pmin[d])
    best = jnp.concatenate([best, jnp.zeros((96, 128), f32)], axis=0)
    out_ref[32:, :128] = jnp.transpose(best)[:8]


def scan(traits, covariates, genotypes, shuffles, samples):
    perms = shuffles.shape[0]
    mats = perms + 1
    ringed = perms - 0
    rows = traits.shape[0]
    vmem = pl.BlockSpec(memory_space=pltpu.VMEM)
    dma = pltpu.SemaphoreType.DMA
    return pl.pallas_call(
        functools.partial(scan_kernel, samples=samples),
        out_shape=jax.ShapeDtypeStruct((40, 256), f32),
        in_specs=[pl.BlockSpec(memory_space=pl.ANY)] * 4,
        out_specs=vmem,
        scratch_shapes=[
            pltpu.VMEM(traits.shape, bf16),
            pltpu.VMEM(covariates.shape[::-1], bf16),
            pltpu.VMEM(genotypes.shape, jnp.int32),
            pltpu.VMEM(shuffles.shape, jnp.int32),
            dma((7,)),
            pltpu.VMEM((1024, rows), bf16),
            pltpu.VMEM((mats, rows, 384), bf16),
            pltpu.VMEM((48, rows), bf16),
            pltpu.VMEM((32, 32, 128), f32),
            pltpu.VMEM((2, mats + 1, 4, 2, 4, 32, 128), f32),
            pltpu.VMEM((2, mats + 1, 6, 4, 32, 128), f32),
            pltpu.VMEM((2, mats + 1, 4, 2, 32, 128), f32),
            pltpu.VMEM((2, ringed, 6, 32, 128), f32),
            pltpu.VMEM((2, mats + 1, 2, 32, 128), f32),
            pltpu.VMEM((2, mats, 32, 128), f32),
            pltpu.VMEM((2, mats + 1 - ringed, 3, 2, 32, 128), f32),
            pltpu.VMEM((2, 32, 128), f32),
            pltpu.VMEM((4, 4, 2, 24, 128), f32),
            pltpu.VMEM((8, 8, 128), f32),
            pltpu.VMEM((mats * 72, 128), f32),
            pltpu.VMEM((128, mats * 256), f32),
            pltpu.VMEM((mats, 32, 256), f32),
            pltpu.VMEM((32, 128), f32),
            pltpu.VMEM((8, 256), f32),
            pltpu.VMEM((32, 128), f32),
            pltpu.VMEM((7, 32, 128), f32),
            dma((2,)), dma((2, mats + 1, 3)),
            dma((2,)), dma((2, ringed, 3)),
            dma((2,)), dma((2, mats)),
            dma((2,)), dma((2, mats + 1 - ringed)),
            dma((5,)), dma((5,)),
        ],
        compiler_params=pltpu.CompilerParams(
            collective_id=0, has_side_effects=True, vmem_limit_bytes=56 * 1024 * 1024
        ),
    )(traits, covariates.T, genotypes, shuffles)


def shards(traits, covariates, genotypes, shuffles):
    samples = traits.shape[0] * lax.axis_size("samp")
    out = scan(traits, covariates, genotypes, shuffles, samples)
    return (out[:32], out[32 : 32 + shuffles.shape[0], :32])


def solution(mesh):
    placed = (P("samp", None), P("samp", None), P("samp", "tile"), P(None, "samp"))
    return jax.shard_map(
        shards,
        mesh=mesh,
        in_specs=placed,
        out_specs=(P("samp", "tile"), P(None, "samp")),
        check_vma=False,
    )
```

```python
import functools
import math

import jax
import jax.numpy as jnp
from jax import lax
from jax.experimental import pallas as pl
from jax.experimental.pallas import tpu as pltpu
from jax.sharding import PartitionSpec as P

C = 32


epsilon = 1e-05
MESH = pl.DeviceIdType.MESH
f32 = jnp.float32
bf16 = jnp.bfloat16


ORDER = (
    "C0", "B", "10", "P1", "C1", "11", "P3", "g1", "P2", "200", "C3", "13",
    "P5", "C2", "P4", "12", "aux", "A1", "210", "C5", "g2", "201", "220", "A2",
    "221", "C4", "211", "15", "231", "A3", "250", "230", "310", "321", "311", "C6",
    "A4", "14", "320", "301", "300", "g3", "331", "330", "410", "241", "421", "240",
    "251", "411", "A5", "400", "401", "16", "inv", "341", "431", "430", "420", "d51",
    "510", "260", "521", "340", "501", "441", "500", "d50", "261", "A6", "531", "530",
    "511", "440", "520", "d60", "e51", "541", "ct", "e50", "d61", "540", "corr", "f1",
    "f0", "f2", "e60", "e61", "f5", "f4", "f3", "T", "f6",
)


def exact_dot(a, b):
    return jnp.dot(a, b, preferred_element_type=f32, precision=lax.Precision.HIGHEST)


def split(a):
    high = a.astype(bf16)
    rest = a - high.astype(f32)
    middle = rest.astype(bf16)
    return high, middle, (rest - middle.astype(f32)).astype(bf16)


def across(a, b):
    return lax.dot_general(a, b, (((1,), (1,)), ((), ())), preferred_element_type=f32)


def iota(shape, dim):
    return lax.broadcasted_iota(jnp.int32, shape, dim)


def scan_kernel(
    y_hbm, cov_hbm, geno_hbm, order_hbm, out_ref,
    y_ref, cov_ref, geno_ref, order_ref, load,
    yt, q, xt, tps, part, in1, mid, in2, low, inz, ind,
    apart, ain1, amid, aind, alow, alowin, agu, tt, gsum, gin,
    inv_ref, ct_ref, lhs, vst, corr, st_ref, sg_ref, pm, pmin,
    send1, recv1, send2, recv2, sendz, recvz, sendd, recvd, sendx, recvx,
    *, samples,
):
    perms = order_hbm.shape[0]
    mats = perms + 1
    own = perms
    aux = mats
    ringed = perms - 1
    rows = y_hbm.shape[0]
    s = lax.axis_index("samp")
    t = lax.axis_index("tile")
    x = lax.rem(s, 4)
    zh = lax.rem(s // 4, 2)
    y = s // 8
    core = lax.rem(t, 2)
    zl = t // 2
    base = s * rows

    def at_x(d):
        return s - x + lax.rem(x + d, 4)

    def at_y(d):
        return lax.rem(s + 8 * d, 32)

    z_peer = s + 4 - 8 * zh

    place = (x, y)
    along = (at_x, at_y)

    barrier = pltpu.get_barrier_semaphore()
    met = [at_y(d) for d in (1, 2, 3)] + [at_x(d) for d in (1, 2, 3)] + [z_peer]
    for peer in met:
        pl.semaphore_signal(barrier, inc=1, device_id={"samp": peer}, device_id_type=MESH)
    for d in range(1, 8):
        pl.semaphore_signal(
            barrier, inc=1, device_id={"tile": lax.rem(t + d, 8)}, device_id_type=MESH
        )

    loads = [
        pltpu.make_async_copy(a, b, load.at[k])
        for k, (a, b) in enumerate(
            [(cov_hbm, cov_ref), (geno_hbm, geno_ref), (order_hbm, order_ref)]
            + [(y_hbm.at[:, pl.ds(k, 256)], y_ref.at[:, pl.ds(k, 256)]) for k in range(0, 1024, 256)]
        )
    ]
    for copy in loads:
        copy.start()

    def remote(src, dst, send, recv, peer):
        return pltpu.make_async_remote_copy(
            src_ref=src, dst_ref=dst, send_sem=send, recv_sem=recv,
            device_id={"samp": peer}, device_id_type=MESH,
        )

    def to_tile(src, dst, k, d):
        return pltpu.make_async_remote_copy(
            src_ref=src, dst_ref=dst, send_sem=sendx.at[k], recv_sem=recvx.at[k],
            device_id={"tile": lax.rem(t + d, 8)}, device_id_type=MESH,
        )

    def all_of(ref, send, recv):
        return remote(ref, ref, send, recv, at_x(1))

    def ring_copy(src, buf, k, c, peers, send, recv):
        blk = lax.rem(c + (2, 2, 1, 3, 1, 3)[k], 4)
        uv = (0, 1, 1, 0, 0, 1)[k]
        ref = buf.at[k - 4] if k >= 4 else src.at[blk, uv]
        return remote(ref, buf.at[k], send, recv.at[min(k, 2)], peers((1, 3, 1, 3, 1, 3)[k]))

    def part_of(h, m):
        return apart if m == aux else part.at[h, m]

    def in1_of(h, m):
        return ain1 if m == aux else in1.at[h, m]

    def mid_of(h, m):
        return amid if m == aux else mid.at[h, m]

    def ind_of(h, m):
        return aind if m == aux else ind.at[h, m - ringed]

    def low_of(h, m):
        return alow if m == aux else low.at[h, m]

    def first_copy(h, m, k):
        return ring_copy(
            part_of(h, m), in1_of(h, m), k, place[h], along[h],
            send1.at[2 if m == aux else h], recv1.at[h, m],
        )

    def second_copy(h, m, k):
        return ring_copy(
            mid.at[h, m], in2.at[h, m], k, place[1 - h], along[1 - h], send2.at[h],
            recv2.at[h, m],
        )

    def z_copy(h, m):
        return remote(
            low.at[h, m, 1 - zh], inz.at[h, m], sendz.at[h], recvz.at[h, m], z_peer
        )

    def compute(m):
        out = jnp.dot(yt[...], q[m, :, :256], preferred_element_type=f32)
        for o in range(32):
            yb, z, xb = o // 8, o // 4 % 2, o % 4
            piece = out[o * 32 : o * 32 + 32]
            part[0, m, xb, z, yb] = piece[:, :128]
            part[1, m, yb, z, xb] = piece[:, 128:]

    def permute(m):
        order = order_ref[pl.ds(m, 1), :] - base
        hot = jnp.where(iota((rows, rows), 0) == order, 1.0, 0.0).astype(bf16)
        q[m] = jnp.dot(hot, q[own], preferred_element_type=f32).astype(bf16)

    def stage1(m, halves=(0, 1)):
        for k in range(4):
            for h in halves:
                first_copy(h, m, k).start()

    def stage2(m, halves=(0, 1)):
        for h in halves:
            c = place[h]
            lines, buf = part_of(h, m), in1_of(h, m)
            for k, d, uv in ((0, 1, 0), (1, 3, 1)):
                first_copy(h, m, k).wait_recv()
                buf[k] = buf[k] + lines[lax.rem(c + d, 4), uv]
                first_copy(h, m, k + 4).start()

    def first_sum(h, m):
        c = place[h]
        lines, buf, to = part_of(h, m), in1_of(h, m), mid_of(h, m)
        all_of(buf.at[pl.ds(2, 4)], send1.at[h], recv1.at[h, m, 2]).wait_recv()
        to[:, 0] = lines[c, 0] + buf[3] + buf[4]
        to[:, 1] = lines[c, 1] + buf[2] + buf[5]

    def stage3(m, halves=(0, 1)):
        for h in halves:
            first_sum(h, m)
            for k in range(4):
                second_copy(h, m, k).start()

    def stage4(m, halves=(0, 1)):
        for h in halves:
            c = place[1 - h]
            for k, d, uv in ((0, 1, 0), (1, 3, 1)):
                second_copy(h, m, k).wait_recv()
                in2[h, m, k] = in2[h, m, k] + mid[h, m, lax.rem(c + d, 4), uv]
                second_copy(h, m, k + 4).start()

    def stage5(m, halves=(0, 1)):
        for h in halves:
            c = place[1 - h]
            all_of(in2.at[h, m, pl.ds(2, 4)], send2.at[h], recv2.at[h, m, 2]).wait_recv()
            low[h, m, 0] = mid[h, m, c, 0] + in2[h, m, 3] + in2[h, m, 4]
            low[h, m, 1] = mid[h, m, c, 1] + in2[h, m, 2] + in2[h, m, 5]
            z_copy(h, m).start()


    def direct(m, halves=(0, 1)):
        for h in halves:
            first_sum(h, m)
            for d in (1, 3, 2):
                remote(
                    mid_of(h, m).at[lax.rem(place[1 - h] + d, 4)], ind_of(h, m).at[d - 1],
                    sendd.at[2 if m == aux else h], recvd.at[h, m - ringed], along[1 - h](d),
                ).start()

    def direct_sum(h, m):
        buf = ind_of(h, m)
        all_of(buf, sendd.at[h], recvd.at[h, m - ringed]).wait_recv()
        total = mid_of(h, m)[place[1 - h]] + buf[0] + buf[1] + buf[2]
        low_of(h, m)[...] = total

    def stage5d(m, halves=(0, 1)):
        for h in halves:
            direct_sum(h, m)
            z_copy(h, m).start()


    def spread_of(m):
        return q[m, :, 256:].astype(f32)

    def aux_parts():
        for m in range(mats):
            out = jnp.dot(xt[...], q[m, :, :256], preferred_element_type=f32)
            for j in range(4):
                for k in range(2):
                    apart[m // 2, m % 2, j, 8 + 8 * k : 16 + 8 * k] = out[
                        8 * j : 8 * j + 8, 128 * k : 128 * k + 128
                    ]
        group = iota((rows, 128), 1) // 32
        picked = []
        for k in range(2):
            value = spread_of(3) if k == 0 else jnp.where(
                iota((rows, 128), 1) == 96, 1.0, 0.0
            )
            for j in range(3):
                value = jnp.where(group == j, spread_of(4 * k + j), value)
            picked.append(value)
            out = jnp.dot(xt[...], value.astype(bf16), preferred_element_type=f32)
            for j in range(4):
                apart[3, 1, j, 8 + 8 * k : 16 + 8 * k] = out[8 * j : 8 * j + 8]
        mine = jnp.where(core == 0, picked[0], picked[1]).astype(bf16)
        out = jnp.dot(yt[...], mine, preferred_element_type=f32)
        wide = yt[...].astype(f32)
        square_at = (iota((1024, 128), 1) == 97) & (core == 1)
        out = jnp.where(square_at, jnp.sum(wide * wide, axis=1, keepdims=True), out)
        tps[...] = out.reshape(32, 32, 128)
        ours = tps[:, pl.ds(pl.multiple_of(zl * 8, 8), 8), :]
        apart[:, :, :, 0:8] = ours.reshape(4, 2, 4, 8, 128)

    def both_copy():
        return remote(alow, alowin, sendx.at[4], recvx.at[4], z_peer)

    def aux_low():
        direct_sum(1, aux)
        both_copy().start()

    def aux_total():
        both_copy().wait_recv()
        total = alow[...] + alowin[...]
        agu[x, y] = total[:, 8:]
        for d in (1, 3, 2):
            remote(agu.at[x, y], agu.at[x, y], sendx.at[2], recvx.at[2], at_y(d)).start()
        tt[t] = jnp.where(zh == 0, total[0, :8], total[1, :8])
        for d in range(1, 8):
            to_tile(tt.at[t], tt.at[t], 0, d).start()

    def aux_row():
        all_of(agu.at[x, pl.ds(0, 3)], sendx.at[2], recvx.at[2]).wait_recv()
        for d in (1, 3, 2):
            remote(agu.at[x], agu.at[x], sendx.at[3], recvx.at[3], at_x(d)).start()


    def gram_send(n):
        for d in (1, 3, 2) if n < 2 else (0,):
            peer = z_peer if n == 2 else along[n](d)
            remote(
                gsum.at[n], gin.at[3 * n + max(d - 1, 0)], sendx.at[5 + n], recvx.at[5 + n], peer
            ).start()

    def gram_start():
        lane = iota((rows, 128), 1)
        wide = jnp.where(lane < 32, spread_of(own), jnp.where(lane == 32, 1.0, 0.0))
        out = jnp.dot(xt[...], wide.astype(bf16), preferred_element_type=f32)[:40]
        geno = q[own, :, :256].astype(f32)
        row = iota((40, 128), 0)
        for k in range(2):
            half = geno[:, 128 * k : 128 * k + 128]
            out = jnp.where(row == 33 + k, jnp.sum(half, axis=0, keepdims=True), out)
            out = jnp.where(row == 35 + k, jnp.sum(half * half, axis=0, keepdims=True), out)
        gsum[0] = out
        gram_send(0)

    def gram_pass(n):
        count = 1 if n == 3 else 3
        at = 3 * n - 3
        all_of(gin.at[pl.ds(at, count)], sendx.at[4 + n], recvx.at[4 + n]).wait_recv()
        total = gsum[n - 1]
        for k in range(count):
            total = total + gin[at + k]
        gsum[n] = total
        if n < 3:
            gram_send(n)

    def invert():
        gram_pass(3)
        lane40 = iota((40, 128), 1)
        row40 = iota((40, 128), 0)
        inv = jnp.where(row40 < C + 1, gsum[3], 0.0)
        for k in range(C + 1):
            pivot = inv[k : k + 1, k : k + 1]
            line = jnp.where(lane40[:1] == k, 1.0, inv[k : k + 1, :]) / pivot
            column = inv[:, k : k + 1]
            rest = jnp.where(lane40 == k, 0.0, inv)
            inv = jnp.where(row40 == k, line, rest - column * line)
        inv_ref[:40] = inv
        inv_ref[40:] = jnp.zeros((88, 128), f32)

    def trait_side():
        all_of(tt.at[pl.ds(0, 7)], sendx.at[0], recvx.at[0]).wait_recv()
        lane = iota((32, 128), 1)
        sums = [jnp.concatenate([tt[2 * k + c] for k in range(4)], axis=0) for c in range(2)]
        ones_y = sums[1][:, 96:97]
        squares_y = sums[1][:, 97:98]
        for m in range(mats):
            mine = sums[m // 4]
            k = m % 4
            if k:
                mine = pltpu.roll(mine, 128 - 32 * k, 1)
            mine = jnp.where(lane < 32, mine, jnp.where(lane == 32, ones_y, 0.0))
            lhs[mats * 40 + m * 32 : mats * 40 + m * 32 + 32] = mine
        coef_t = exact_dot(mine, inv_ref[...])
        coef_t = coef_t.astype(bf16).astype(f32)
        ct_ref[...] = coef_t
        gram = jnp.where(iota((40, 128), 0) < C + 1, gsum[3], 0.0)
        back = exact_dot(coef_t, jnp.concatenate([gram, jnp.zeros((88, 128), f32)], axis=0))
        squares_t = squares_y - jnp.sum(coef_t * (2.0 * mine - back), axis=1, keepdims=True)
        mean_t = jnp.maximum(squares_t, 0.0) / samples
        factor_z = math.sqrt(samples - C - 2) / samples
        st_ref[...] = jnp.broadcast_to(lax.rsqrt(mean_t + epsilon) * factor_z, (32, 128))

    def corrections():
        all_of(agu.at[pl.ds(0, 3)], sendx.at[3], recvx.at[3]).wait_recv()
        lane = iota((32, 128), 1)

        def product(m, k):
            return agu[:, m // 2, m % 2, 8 * k : 8 * k + 8].reshape(32, 128)

        gram = gsum[3]
        first = iota((8, 128), 0) == 0
        last_rows = jnp.where(first, gram[32:40], 0.0)
        ones_g = jnp.concatenate([gram[33:34], gram[34:35]], axis=1)
        squares_g = jnp.concatenate([gram[35:36], gram[36:37]], axis=1)
        ones_rows = jnp.where(iota((8, 256), 0) == 0, ones_g, 0.0)
        spreads = [product(7, 0), product(7, 1)]

        def geno_of(m):
            body = jnp.concatenate([product(m, 0), product(m, 1)], axis=1)
            return jnp.concatenate([body, ones_rows], axis=0)

        for m in range(mats):
            if m == own:
                body = gram[:32]
            else:
                body = spreads[m // 4]
                if m % 4:
                    body = pltpu.roll(body, 128 - 32 * (m % 4), 1)
                body = jnp.where(lane < 32, body, jnp.where(lane == 32, gram[:32], 0.0))
            lhs[m * 40 : m * 40 + 32] = body
            lhs[m * 40 + 32 : m * 40 + 40] = last_rows
        geno0 = geno_of(own)
        pad256 = jnp.zeros((88, 256), f32)
        coef_g = exact_dot(inv_ref[:40], jnp.concatenate([geno0, pad256], axis=0))
        rounded_g = jnp.concatenate([coef_g, pad256], axis=0).astype(bf16)
        coef_g = coef_g.astype(bf16).astype(f32)
        rounded_t = ct_ref[...].astype(bf16)
        out = sum(
            jnp.dot(piece, rounded_g, preferred_element_type=f32) for piece in split(lhs[...])
        )
        for m in range(mats):
            left = geno_of(m) - out[m * 40 : m * 40 + 40]
            vst[:40, m * 256 : m * 256 + 256] = left
            vst[40:, m * 256 : m * 256 + 256] = jnp.zeros((8, 256), f32)
            if m == own:
                squares_g = squares_g - jnp.sum(
                    coef_g * (geno0 + left), axis=0, keepdims=True
                )
        more = sum(
            jnp.dot(rounded_t[:, :48], piece, preferred_element_type=f32)
            for piece in split(vst[...])
        )
        for m in range(mats):
            at = mats * 40 + m * 32
            corr[m] = out[at : at + 32] + more[:, m * 256 : m * 256 + 256]
        mean_g = jnp.maximum(squares_g, 0.0) / samples
        sg_ref[...] = jnp.broadcast_to(lax.rsqrt(mean_g + epsilon), (8, 256))

    def owned(m):
        outs = []
        for h in range(2):
            z_copy(h, m).wait_recv()
            total = low[h, m, zh] + inz[h, m]
            cols = slice(h * 128, h * 128 + 128)
            outs.append((total - corr[m, :, cols]) * st_ref[...] * sg_ref[0:1, cols])
        return outs

    loads[0].wait()
    loads[1].wait()
    spread = jnp.where(lax.rem(iota((32, 128), 1), 32) == iota((32, 128), 0), 1.0, 0.0)
    spread = spread.astype(bf16)
    for b in range(4):
        at = slice(b * 256, b * 256 + 256)
        q[own, at, :256] = geno_ref[at, :].astype(f32).astype(bf16)
        q[own, at, 256:] = lax.dot_general(
            cov_ref[:, at], spread, (((0,), (0,)), ((), ())), preferred_element_type=f32
        ).astype(bf16)
    xt[:32] = cov_ref[...]
    xt[32:] = jnp.where(iota((16, rows), 0) == 0, 1.0, 0.0).astype(bf16)
    eye = jnp.where(iota((256, 256), 0) == iota((256, 256), 1), 1.0, 0.0).astype(bf16)

    loads[2].wait()
    permute(0)
    for b in range(4):
        loads[3 + b].wait()
        at = slice(b * 256, b * 256 + 256)
        yt[at, :] = across(eye, y_ref[:, at]).astype(bf16)

    lane = iota((32, 128), 1)
    held = {"best": jnp.zeros((32, 128), f32)}

    def finish(m):
        left, right = owned(m)
        if m == own:
            out_ref[:32, :128] = left
            out_ref[:32, 128:] = right
            out_ref[32:, 128:] = jnp.zeros((8, 128), f32)
            return
        peak = jnp.max(jnp.maximum(jnp.abs(left), jnp.abs(right)), axis=1, keepdims=True)
        held["best"] = jnp.where(lane == m, peak, held["best"])

    def exchange():
        pm[...] = held["best"]
        for d in range(1, 8):
            to_tile(pm, pmin.at[d - 1], 1, d).start()

    stages = {"2": stage2, "3": stage3, "4": stage4, "5": stage5, "d": direct, "e": stage5d}
    whole = {"P": permute, "C": compute, "1": stage1, "f": finish}
    single = {
        "aux": aux_parts,
        "A1": lambda: stage1(aux, (1,)),
        "A2": lambda: stage2(aux, (1,)),
        "A3": lambda: direct(aux, (1,)),
        "A4": aux_low,
        "A5": aux_total,
        "A6": aux_row,
        "inv": invert,
        "ct": trait_side,
        "corr": corrections,
        "g1": gram_start,
        "g2": lambda: gram_pass(1),
        "g3": lambda: gram_pass(2),
        "T": exchange,
        "B": lambda: pl.semaphore_wait(barrier, len(met) + 7),
    }
    for name in ORDER:
        if name in single:
            single[name]()
        elif name[0] in whole:
            whole[name[0]](int(name[1]))
        else:
            stages[name[0]](int(name[1]), (int(name[2]),))
    best = held["best"]

    for h in range(2):
        all_of(in1.at[h], send1.at[h], recv1.at[0, 0, 0]).wait_send()
        all_of(in2.at[h], send2.at[h], recv2.at[0, 0, 0]).wait_send()
        all_of(inz.at[h], sendz.at[h], recvz.at[0, 0]).wait_send()
        all_of(ind.at[h], sendd.at[h], recvd.at[0, 0]).wait_send()
    all_of(tt.at[pl.ds(0, 7)], sendx.at[0], recvx.at[0]).wait_send()
    all_of(agu.at[x, pl.ds(0, 3)], sendx.at[2], recvx.at[2]).wait_send()
    both_copy().wait_send()
    all_of(ain1, send1.at[2], recv1.at[0, 0, 0]).wait_send()
    all_of(aind, sendd.at[2], recvd.at[0, 0]).wait_send()
    for n in range(3):
        sent = gin.at[pl.ds(0, 3 if n < 2 else 1)]
        all_of(sent, sendx.at[5 + n], recvx.at[5 + n]).wait_send()
    all_of(agu.at[pl.ds(0, 3)], sendx.at[3], recvx.at[3]).wait_send()
    all_of(pmin, sendx.at[1], recvx.at[1]).wait()
    for d in range(7):
        best = jnp.maximum(best, pmin[d])
    best = jnp.concatenate([best, jnp.zeros((96, 128), f32)], axis=0)
    out_ref[32:, :128] = jnp.transpose(best)[:8]


def scan(traits, covariates, genotypes, shuffles, samples):
    perms = shuffles.shape[0]
    mats = perms + 1
    ringed = perms - 1
    rows = traits.shape[0]
    vmem = pl.BlockSpec(memory_space=pltpu.VMEM)
    dma = pltpu.SemaphoreType.DMA
    return pl.pallas_call(
        functools.partial(scan_kernel, samples=samples),
        out_shape=jax.ShapeDtypeStruct((40, 256), f32),
        in_specs=[pl.BlockSpec(memory_space=pl.ANY)] * 4,
        out_specs=vmem,
        scratch_shapes=[
            pltpu.VMEM(traits.shape, bf16),
            pltpu.VMEM(covariates.shape[::-1], bf16),
            pltpu.VMEM(genotypes.shape, jnp.int32),
            pltpu.VMEM(shuffles.shape, jnp.int32),
            dma((7,)),
            pltpu.VMEM((1024, rows), bf16),
            pltpu.VMEM((mats, rows, 384), bf16),
            pltpu.VMEM((48, rows), bf16),
            pltpu.VMEM((32, 32, 128), f32),
            pltpu.VMEM((2, mats, 4, 2, 4, 32, 128), f32),
            pltpu.VMEM((2, mats, 6, 4, 32, 128), f32),
            pltpu.VMEM((2, mats, 4, 2, 32, 128), f32),
            pltpu.VMEM((2, ringed, 6, 32, 128), f32),
            pltpu.VMEM((2, mats, 2, 32, 128), f32),
            pltpu.VMEM((2, mats, 32, 128), f32),
            pltpu.VMEM((2, mats - ringed, 3, 2, 32, 128), f32),
            pltpu.VMEM((4, 2, 4, 24, 128), f32),
            pltpu.VMEM((6, 4, 24, 128), f32),
            pltpu.VMEM((4, 2, 24, 128), f32),
            pltpu.VMEM((3, 2, 24, 128), f32),
            pltpu.VMEM((2, 24, 128), f32),
            pltpu.VMEM((2, 24, 128), f32),
            pltpu.VMEM((4, 4, 2, 16, 128), f32),
            pltpu.VMEM((8, 8, 128), f32),
            pltpu.VMEM((4, 40, 128), f32),
            pltpu.VMEM((7, 40, 128), f32),
            pltpu.VMEM((128, 128), f32),
            pltpu.VMEM((32, 128), f32),
            pltpu.VMEM((mats * 72, 128), f32),
            pltpu.VMEM((48, mats * 256), f32),
            pltpu.VMEM((mats, 32, 256), f32),
            pltpu.VMEM((32, 128), f32),
            pltpu.VMEM((8, 256), f32),
            pltpu.VMEM((32, 128), f32),
            pltpu.VMEM((7, 32, 128), f32),
            dma((3,)), dma((2, mats + 1, 3)),
            dma((2,)), dma((2, ringed, 3)),
            dma((2,)), dma((2, mats)),
            dma((3,)), dma((2, mats + 1 - ringed)),
            dma((8,)), dma((8,)),
        ],
        compiler_params=pltpu.CompilerParams(
            collective_id=0, has_side_effects=True, vmem_limit_bytes=56 * 1024 * 1024
        ),
    )(traits, covariates.T, genotypes, shuffles)


def shards(traits, covariates, genotypes, shuffles):
    samples = traits.shape[0] * lax.axis_size("samp")
    out = scan(traits, covariates, genotypes, shuffles, samples)
    return (out[:32], out[32 : 32 + shuffles.shape[0], :32])


def solution(mesh):
    placed = (P("samp", None), P("samp", None), P("samp", "tile"), P(None, "samp"))
    return jax.shard_map(
        shards,
        mesh=mesh,
        in_specs=placed,
        out_specs=(P("samp", "tile"), P(None, "samp")),
        check_vma=False,
    )
```

```python
import functools
import math

import jax
import jax.numpy as jnp
from jax import lax
from jax.experimental import pallas as pl
from jax.experimental.pallas import tpu as pltpu
from jax.sharding import PartitionSpec as P

C = 32


epsilon = 1e-05
MESH = pl.DeviceIdType.MESH
f32 = jnp.float32
bf16 = jnp.bfloat16


ORDER = (
    "C0", "B", "10", "g1", "P1", "C1", "11", "P2", "C2", "201", "P4", "12",
    "P3", "C4", "14", "P5", "aux", "A1", "301", "200", "C3", "13", "210", "240",
    "A2", "241", "401", "211", "221", "C5", "230", "A3", "15", "340", "341", "310",
    "231", "311", "321", "C6", "A4", "220", "251", "g2", "16", "501", "441", "300",
    "440", "331", "421", "250", "330", "411", "260", "A5", "320", "431", "261", "g3",
    "d51", "521", "541", "540", "410", "400", "d50", "420", "511", "430", "A6", "531",
    "d61", "510", "d60", "500", "e51", "520", "530", "e50", "inv", "ct", "e61", "e60",
    "corr", "f4", "f2", "f1", "f0", "f3", "f5", "T", "f6",
)


def exact_dot(a, b):
    return jnp.dot(a, b, preferred_element_type=f32, precision=lax.Precision.HIGHEST)


def split(a):
    high = a.astype(bf16)
    rest = a - high.astype(f32)
    middle = rest.astype(bf16)
    return high, middle, (rest - middle.astype(f32)).astype(bf16)


def across(a, b):
    return lax.dot_general(a, b, (((1,), (1,)), ((), ())), preferred_element_type=f32)


def iota(shape, dim):
    return lax.broadcasted_iota(jnp.int32, shape, dim)


def scan_kernel(
    y_hbm, cov_hbm, geno_hbm, order_hbm, out_ref,
    y_ref, cov_ref, geno_ref, order_ref, load,
    yt, q, xt, tps, part, in1, mid, in2, low, inz, ind,
    apart, ain1, amid, aind, alow, alowin, agu, tt, gsum, gin,
    inv_ref, ct_ref, lhs, vst, corr, st_ref, sg_ref, pm, pmin,
    send1, recv1, send2, recv2, sendz, recvz, sendd, recvd, sendx, recvx,
    *, samples,
):
    perms = order_hbm.shape[0]
    mats = perms + 1
    own = perms
    aux = mats
    ringed = perms - 1
    rows = y_hbm.shape[0]
    s = lax.axis_index("samp")
    t = lax.axis_index("tile")
    x = lax.rem(s, 4)
    zh = lax.rem(s // 4, 2)
    y = s // 8
    core = lax.rem(t, 2)
    zl = t // 2
    base = s * rows

    def at_x(d):
        return s - x + lax.rem(x + d, 4)

    def at_y(d):
        return lax.rem(s + 8 * d, 32)

    z_peer = s + 4 - 8 * zh

    place = (x, y)
    along = (at_x, at_y)

    barrier = pltpu.get_barrier_semaphore()
    met = [at_y(d) for d in (1, 2, 3)] + [at_x(d) for d in (1, 2, 3)] + [z_peer]
    for peer in met:
        pl.semaphore_signal(barrier, inc=1, device_id={"samp": peer}, device_id_type=MESH)
    for d in range(1, 8):
        pl.semaphore_signal(
            barrier, inc=1, device_id={"tile": lax.rem(t + d, 8)}, device_id_type=MESH
        )

    loads = [
        pltpu.make_async_copy(a, b, load.at[k])
        for k, (a, b) in enumerate(
            [(cov_hbm, cov_ref), (geno_hbm, geno_ref), (order_hbm, order_ref)]
            + [(y_hbm.at[:, pl.ds(k, 256)], y_ref.at[:, pl.ds(k, 256)]) for k in range(0, 1024, 256)]
        )
    ]
    for copy in loads:
        copy.start()

    def remote(src, dst, send, recv, peer):
        return pltpu.make_async_remote_copy(
            src_ref=src, dst_ref=dst, send_sem=send, recv_sem=recv,
            device_id={"samp": peer}, device_id_type=MESH,
        )

    def to_tile(src, dst, k, d):
        return pltpu.make_async_remote_copy(
            src_ref=src, dst_ref=dst, send_sem=sendx.at[k], recv_sem=recvx.at[k],
            device_id={"tile": lax.rem(t + d, 8)}, device_id_type=MESH,
        )

    def all_of(ref, send, recv):
        return remote(ref, ref, send, recv, at_x(1))

    def ring_copy(src, buf, k, c, peers, send, recv):
        blk = lax.rem(c + (2, 2, 1, 3, 1, 3)[k], 4)
        uv = (0, 1, 1, 0, 0, 1)[k]
        ref = buf.at[k - 4] if k >= 4 else src.at[blk, uv]
        return remote(ref, buf.at[k], send, recv.at[min(k, 2)], peers((1, 3, 1, 3, 1, 3)[k]))

    def part_of(h, m):
        return apart if m == aux else part.at[h, m]

    def in1_of(h, m):
        return ain1 if m == aux else in1.at[h, m]

    def mid_of(h, m):
        return amid if m == aux else mid.at[h, m]

    def ind_of(h, m):
        return aind if m == aux else ind.at[h, m - ringed]

    def low_of(h, m):
        return alow if m == aux else low.at[h, m]

    def first_copy(h, m, k):
        return ring_copy(
            part_of(h, m), in1_of(h, m), k, place[h], along[h],
            send1.at[2 if m == aux else h], recv1.at[h, m],
        )

    def second_copy(h, m, k):
        return ring_copy(
            mid.at[h, m], in2.at[h, m], k, place[1 - h], along[1 - h], send2.at[h],
            recv2.at[h, m],
        )

    def z_copy(h, m):
        return remote(
            low.at[h, m, 1 - zh], inz.at[h, m], sendz.at[h], recvz.at[h, m], z_peer
        )

    def compute(m):
        out = jnp.dot(yt[...], q[m, :, :256], preferred_element_type=f32)
        for o in range(32):
            yb, z, xb = o // 8, o // 4 % 2, o % 4
            piece = out[o * 32 : o * 32 + 32]
            part[0, m, xb, z, yb] = piece[:, :128]
            part[1, m, yb, z, xb] = piece[:, 128:]

    def permute(m):
        order = order_ref[pl.ds(m, 1), :] - base
        hot = jnp.where(iota((rows, rows), 0) == order, 1.0, 0.0).astype(bf16)
        q[m] = jnp.dot(hot, q[own], preferred_element_type=f32).astype(bf16)

    def stage1(m, halves=(0, 1)):
        for k in range(4):
            for h in halves:
                first_copy(h, m, k).start()

    def stage2(m, halves=(0, 1)):
        for h in halves:
            c = place[h]
            lines, buf = part_of(h, m), in1_of(h, m)
            for k, d, uv in ((0, 1, 0), (1, 3, 1)):
                first_copy(h, m, k).wait_recv()
                buf[k] = buf[k] + lines[lax.rem(c + d, 4), uv]
                first_copy(h, m, k + 4).start()

    def first_sum(h, m):
        c = place[h]
        lines, buf, to = part_of(h, m), in1_of(h, m), mid_of(h, m)
        all_of(buf.at[pl.ds(2, 4)], send1.at[h], recv1.at[h, m, 2]).wait_recv()
        to[:, 0] = lines[c, 0] + buf[3] + buf[4]
        to[:, 1] = lines[c, 1] + buf[2] + buf[5]

    def stage3(m, halves=(0, 1)):
        for h in halves:
            first_sum(h, m)
            for k in range(4):
                second_copy(h, m, k).start()

    def stage4(m, halves=(0, 1)):
        for h in halves:
            c = place[1 - h]
            for k, d, uv in ((0, 1, 0), (1, 3, 1)):
                second_copy(h, m, k).wait_recv()
                in2[h, m, k] = in2[h, m, k] + mid[h, m, lax.rem(c + d, 4), uv]
                second_copy(h, m, k + 4).start()

    def stage5(m, halves=(0, 1)):
        for h in halves:
            c = place[1 - h]
            all_of(in2.at[h, m, pl.ds(2, 4)], send2.at[h], recv2.at[h, m, 2]).wait_recv()
            low[h, m, 0] = mid[h, m, c, 0] + in2[h, m, 3] + in2[h, m, 4]
            low[h, m, 1] = mid[h, m, c, 1] + in2[h, m, 2] + in2[h, m, 5]
            z_copy(h, m).start()


    def direct(m, halves=(0, 1)):
        for h in halves:
            first_sum(h, m)
            for d in (1, 3, 2):
                remote(
                    mid_of(h, m).at[lax.rem(place[1 - h] + d, 4)], ind_of(h, m).at[d - 1],
                    sendd.at[2 if m == aux else h], recvd.at[h, m - ringed], along[1 - h](d),
                ).start()

    def direct_sum(h, m):
        buf = ind_of(h, m)
        all_of(buf, sendd.at[h], recvd.at[h, m - ringed]).wait_recv()
        total = mid_of(h, m)[place[1 - h]] + buf[0] + buf[1] + buf[2]
        low_of(h, m)[...] = total

    def stage5d(m, halves=(0, 1)):
        for h in halves:
            direct_sum(h, m)
            z_copy(h, m).start()


    def spread_of(m):
        return q[m, :, 256:].astype(f32)

    def aux_parts():
        for m in range(mats):
            out = jnp.dot(xt[...], q[m, :, :256], preferred_element_type=f32)
            for j in range(4):
                for k in range(2):
                    apart[m // 2, m % 2, j, 8 + 8 * k : 16 + 8 * k] = out[
                        8 * j : 8 * j + 8, 128 * k : 128 * k + 128
                    ]
        group = iota((rows, 128), 1) // 32
        picked = []
        for k in range(2):
            value = spread_of(3) if k == 0 else jnp.where(
                iota((rows, 128), 1) == 96, 1.0, 0.0
            )
            for j in range(3):
                value = jnp.where(group == j, spread_of(4 * k + j), value)
            picked.append(value)
            out = jnp.dot(xt[...], value.astype(bf16), preferred_element_type=f32)
            for j in range(4):
                apart[3, 1, j, 8 + 8 * k : 16 + 8 * k] = out[8 * j : 8 * j + 8]
        mine = jnp.where(core == 0, picked[0], picked[1]).astype(bf16)
        out = jnp.dot(yt[...], mine, preferred_element_type=f32)
        wide = yt[...].astype(f32)
        square_at = (iota((1024, 128), 1) == 97) & (core == 1)
        out = jnp.where(square_at, jnp.sum(wide * wide, axis=1, keepdims=True), out)
        tps[...] = out.reshape(32, 32, 128)
        ours = tps[:, pl.ds(pl.multiple_of(zl * 8, 8), 8), :]
        apart[:, :, :, 0:8] = ours.reshape(4, 2, 4, 8, 128)

    def both_copy():
        return remote(alow, alowin, sendx.at[4], recvx.at[4], z_peer)

    def aux_low():
        direct_sum(1, aux)
        both_copy().start()

    def aux_total():
        both_copy().wait_recv()
        total = alow[...] + alowin[...]
        agu[x, y] = total[:, 8:]
        for d in (1, 3, 2):
            remote(agu.at[x, y], agu.at[x, y], sendx.at[2], recvx.at[2], at_y(d)).start()
        tt[t] = jnp.where(zh == 0, total[0, :8], total[1, :8])
        for d in range(1, 8):
            to_tile(tt.at[t], tt.at[t], 0, d).start()

    def aux_row():
        all_of(agu.at[x, pl.ds(0, 3)], sendx.at[2], recvx.at[2]).wait_recv()
        for d in (1, 3, 2):
            remote(agu.at[x], agu.at[x], sendx.at[3], recvx.at[3], at_x(d)).start()


    def gram_send(n):
        for d in (1, 3, 2) if n < 2 else (0,):
            peer = z_peer if n == 2 else along[n](d)
            remote(
                gsum.at[n], gin.at[3 * n + max(d - 1, 0)], sendx.at[5 + n], recvx.at[5 + n], peer
            ).start()

    def gram_start():
        lane = iota((rows, 128), 1)
        wide = jnp.where(lane < 32, spread_of(own), jnp.where(lane == 32, 1.0, 0.0))
        out = jnp.dot(xt[...], wide.astype(bf16), preferred_element_type=f32)[:40]
        geno = q[own, :, :256].astype(f32)
        row = iota((40, 128), 0)
        for k in range(2):
            half = geno[:, 128 * k : 128 * k + 128]
            out = jnp.where(row == 33 + k, jnp.sum(half, axis=0, keepdims=True), out)
            out = jnp.where(row == 35 + k, jnp.sum(half * half, axis=0, keepdims=True), out)
        gsum[0] = out
        gram_send(0)

    def gram_pass(n):
        count = 1 if n == 3 else 3
        at = 3 * n - 3
        all_of(gin.at[pl.ds(at, count)], sendx.at[4 + n], recvx.at[4 + n]).wait_recv()
        total = gsum[n - 1]
        for k in range(count):
            total = total + gin[at + k]
        gsum[n] = total
        if n < 3:
            gram_send(n)

    def invert():
        gram_pass(3)
        lane40 = iota((40, 128), 1)
        row40 = iota((40, 128), 0)
        inv = jnp.where(row40 < C + 1, gsum[3], 0.0)
        for k in range(C + 1):
            pivot = inv[k : k + 1, k : k + 1]
            line = jnp.where(lane40[:1] == k, 1.0, inv[k : k + 1, :]) / pivot
            column = inv[:, k : k + 1]
            rest = jnp.where(lane40 == k, 0.0, inv)
            inv = jnp.where(row40 == k, line, rest - column * line)
        inv_ref[:40] = inv
        inv_ref[40:] = jnp.zeros((88, 128), f32)

    def trait_side():
        all_of(tt.at[pl.ds(0, 7)], sendx.at[0], recvx.at[0]).wait_recv()
        lane = iota((32, 128), 1)
        sums = [jnp.concatenate([tt[2 * k + c] for k in range(4)], axis=0) for c in range(2)]
        ones_y = sums[1][:, 96:97]
        squares_y = sums[1][:, 97:98]
        for m in range(mats):
            mine = sums[m // 4]
            k = m % 4
            if k:
                mine = pltpu.roll(mine, 128 - 32 * k, 1)
            mine = jnp.where(lane < 32, mine, jnp.where(lane == 32, ones_y, 0.0))
            lhs[mats * 40 + m * 32 : mats * 40 + m * 32 + 32] = mine
        coef_t = exact_dot(mine, inv_ref[...])
        coef_t = coef_t.astype(bf16).astype(f32)
        ct_ref[...] = coef_t
        gram = jnp.where(iota((40, 128), 0) < C + 1, gsum[3], 0.0)
        back = exact_dot(coef_t, jnp.concatenate([gram, jnp.zeros((88, 128), f32)], axis=0))
        squares_t = squares_y - jnp.sum(coef_t * (2.0 * mine - back), axis=1, keepdims=True)
        mean_t = jnp.maximum(squares_t, 0.0) / samples
        factor_z = math.sqrt(samples - C - 2) / samples
        st_ref[...] = jnp.broadcast_to(lax.rsqrt(mean_t + epsilon) * factor_z, (32, 128))

    def corrections():
        all_of(agu.at[pl.ds(0, 3)], sendx.at[3], recvx.at[3]).wait_recv()
        lane = iota((32, 128), 1)

        def product(m, k):
            return agu[:, m // 2, m % 2, 8 * k : 8 * k + 8].reshape(32, 128)

        gram = gsum[3]
        first = iota((8, 128), 0) == 0
        last_rows = jnp.where(first, gram[32:40], 0.0)
        ones_g = jnp.concatenate([gram[33:34], gram[34:35]], axis=1)
        squares_g = jnp.concatenate([gram[35:36], gram[36:37]], axis=1)
        ones_rows = jnp.where(iota((8, 256), 0) == 0, ones_g, 0.0)
        spreads = [product(7, 0), product(7, 1)]

        def geno_of(m):
            body = jnp.concatenate([product(m, 0), product(m, 1)], axis=1)
            return jnp.concatenate([body, ones_rows], axis=0)

        for m in range(mats):
            if m == own:
                body = gram[:32]
            else:
                body = spreads[m // 4]
                if m % 4:
                    body = pltpu.roll(body, 128 - 32 * (m % 4), 1)
                body = jnp.where(lane < 32, body, jnp.where(lane == 32, gram[:32], 0.0))
            lhs[m * 40 : m * 40 + 32] = body
            lhs[m * 40 + 32 : m * 40 + 40] = last_rows
        geno0 = geno_of(own)
        pad256 = jnp.zeros((88, 256), f32)
        coef_g = exact_dot(inv_ref[:40], jnp.concatenate([geno0, pad256], axis=0))
        rounded_g = jnp.concatenate([coef_g, pad256], axis=0).astype(bf16)
        coef_g = coef_g.astype(bf16).astype(f32)
        rounded_t = ct_ref[...].astype(bf16)
        out = sum(
            jnp.dot(piece, rounded_g, preferred_element_type=f32) for piece in split(lhs[...])
        )
        for m in range(mats):
            left = geno_of(m) - out[m * 40 : m * 40 + 40]
            vst[:40, m * 256 : m * 256 + 256] = left
            vst[40:, m * 256 : m * 256 + 256] = jnp.zeros((8, 256), f32)
            if m == own:
                squares_g = squares_g - jnp.sum(
                    coef_g * (geno0 + left), axis=0, keepdims=True
                )
        more = sum(
            jnp.dot(rounded_t[:, :48], piece, preferred_element_type=f32)
            for piece in split(vst[...])
        )
        for m in range(mats):
            at = mats * 40 + m * 32
            corr[m] = out[at : at + 32] + more[:, m * 256 : m * 256 + 256]
        mean_g = jnp.maximum(squares_g, 0.0) / samples
        sg_ref[...] = jnp.broadcast_to(lax.rsqrt(mean_g + epsilon), (8, 256))

    def owned(m):
        outs = []
        for h in range(2):
            z_copy(h, m).wait_recv()
            total = low[h, m, zh] + inz[h, m]
            cols = slice(h * 128, h * 128 + 128)
            outs.append((total - corr[m, :, cols]) * st_ref[...] * sg_ref[0:1, cols])
        return outs

    loads[0].wait()
    loads[1].wait()
    spread = jnp.where(lax.rem(iota((32, 128), 1), 32) == iota((32, 128), 0), 1.0, 0.0)
    spread = spread.astype(bf16)
    for b in range(4):
        at = slice(b * 256, b * 256 + 256)
        q[own, at, :256] = geno_ref[at, :].astype(f32).astype(bf16)
        q[own, at, 256:] = lax.dot_general(
            cov_ref[:, at], spread, (((0,), (0,)), ((), ())), preferred_element_type=f32
        ).astype(bf16)
    xt[:32] = cov_ref[...]
    xt[32:] = jnp.where(iota((16, rows), 0) == 0, 1.0, 0.0).astype(bf16)
    eye = jnp.where(iota((256, 256), 0) == iota((256, 256), 1), 1.0, 0.0).astype(bf16)

    loads[2].wait()
    permute(0)
    for b in range(4):
        loads[3 + b].wait()
        at = slice(b * 256, b * 256 + 256)
        yt[at, :] = across(eye, y_ref[:, at]).astype(bf16)

    lane = iota((32, 128), 1)
    held = {"best": jnp.zeros((32, 128), f32)}

    def finish(m):
        left, right = owned(m)
        if m == own:
            out_ref[:32, :128] = left
            out_ref[:32, 128:] = right
            out_ref[32:, 128:] = jnp.zeros((8, 128), f32)
            return
        peak = jnp.max(jnp.maximum(jnp.abs(left), jnp.abs(right)), axis=1, keepdims=True)
        held["best"] = jnp.where(lane == m, peak, held["best"])

    def exchange():
        pm[...] = held["best"]
        for d in range(1, 8):
            to_tile(pm, pmin.at[d - 1], 1, d).start()

    stages = {"2": stage2, "3": stage3, "4": stage4, "5": stage5, "d": direct, "e": stage5d}
    whole = {"P": permute, "C": compute, "1": stage1, "f": finish}
    single = {
        "aux": aux_parts,
        "A1": lambda: stage1(aux, (1,)),
        "A2": lambda: stage2(aux, (1,)),
        "A3": lambda: direct(aux, (1,)),
        "A4": aux_low,
        "A5": aux_total,
        "A6": aux_row,
        "inv": invert,
        "ct": trait_side,
        "corr": corrections,
        "g1": gram_start,
        "g2": lambda: gram_pass(1),
        "g3": lambda: gram_pass(2),
        "T": exchange,
        "B": lambda: pl.semaphore_wait(barrier, len(met) + 7),
    }
    for name in ORDER:
        if name in single:
            single[name]()
        elif name[0] in whole:
            whole[name[0]](int(name[1]))
        else:
            stages[name[0]](int(name[1]), (int(name[2]),))
    best = held["best"]

    for h in range(2):
        all_of(in1.at[h], send1.at[h], recv1.at[0, 0, 0]).wait_send()
        all_of(in2.at[h], send2.at[h], recv2.at[0, 0, 0]).wait_send()
        all_of(inz.at[h], sendz.at[h], recvz.at[0, 0]).wait_send()
        all_of(ind.at[h], sendd.at[h], recvd.at[0, 0]).wait_send()
    all_of(tt.at[pl.ds(0, 7)], sendx.at[0], recvx.at[0]).wait_send()
    all_of(agu.at[x, pl.ds(0, 3)], sendx.at[2], recvx.at[2]).wait_send()
    both_copy().wait_send()
    all_of(ain1, send1.at[2], recv1.at[0, 0, 0]).wait_send()
    all_of(aind, sendd.at[2], recvd.at[0, 0]).wait_send()
    for n in range(3):
        sent = gin.at[pl.ds(0, 3 if n < 2 else 1)]
        all_of(sent, sendx.at[5 + n], recvx.at[5 + n]).wait_send()
    all_of(agu.at[pl.ds(0, 3)], sendx.at[3], recvx.at[3]).wait_send()
    all_of(pmin, sendx.at[1], recvx.at[1]).wait()
    for d in range(7):
        best = jnp.maximum(best, pmin[d])
    best = jnp.concatenate([best, jnp.zeros((96, 128), f32)], axis=0)
    out_ref[32:, :128] = jnp.transpose(best)[:8]


def hand_out(both_ref, obs_ref, peak_ref):
    obs_ref[...] = both_ref[:32]
    peak_ref[...] = both_ref[32 : 32 + peak_ref.shape[0], :32]


def scan(traits, covariates, genotypes, shuffles, samples):
    perms = shuffles.shape[0]
    mats = perms + 1
    ringed = perms - 1
    rows = traits.shape[0]
    vmem = pl.BlockSpec(memory_space=pltpu.VMEM)
    dma = pltpu.SemaphoreType.DMA
    return pl.pallas_call(
        functools.partial(scan_kernel, samples=samples),
        out_shape=jax.ShapeDtypeStruct((40, 256), f32),
        in_specs=[pl.BlockSpec(memory_space=pl.ANY)] * 4,
        out_specs=vmem,
        scratch_shapes=[
            pltpu.VMEM(traits.shape, bf16),
            pltpu.VMEM(covariates.shape[::-1], bf16),
            pltpu.VMEM(genotypes.shape, jnp.int32),
            pltpu.VMEM(shuffles.shape, jnp.int32),
            dma((7,)),
            pltpu.VMEM((1024, rows), bf16),
            pltpu.VMEM((mats, rows, 384), bf16),
            pltpu.VMEM((48, rows), bf16),
            pltpu.VMEM((32, 32, 128), f32),
            pltpu.VMEM((2, mats, 4, 2, 4, 32, 128), f32),
            pltpu.VMEM((2, mats, 6, 4, 32, 128), f32),
            pltpu.VMEM((2, mats, 4, 2, 32, 128), f32),
            pltpu.VMEM((2, ringed, 6, 32, 128), f32),
            pltpu.VMEM((2, mats, 2, 32, 128), f32),
            pltpu.VMEM((2, mats, 32, 128), f32),
            pltpu.VMEM((2, mats - ringed, 3, 2, 32, 128), f32),
            pltpu.VMEM((4, 2, 4, 24, 128), f32),
            pltpu.VMEM((6, 4, 24, 128), f32),
            pltpu.VMEM((4, 2, 24, 128), f32),
            pltpu.VMEM((3, 2, 24, 128), f32),
            pltpu.VMEM((2, 24, 128), f32),
            pltpu.VMEM((2, 24, 128), f32),
            pltpu.VMEM((4, 4, 2, 16, 128), f32),
            pltpu.VMEM((8, 8, 128), f32),
            pltpu.VMEM((4, 40, 128), f32),
            pltpu.VMEM((7, 40, 128), f32),
            pltpu.VMEM((128, 128), f32),
            pltpu.VMEM((32, 128), f32),
            pltpu.VMEM((mats * 72, 128), f32),
            pltpu.VMEM((48, mats * 256), f32),
            pltpu.VMEM((mats, 32, 256), f32),
            pltpu.VMEM((32, 128), f32),
            pltpu.VMEM((8, 256), f32),
            pltpu.VMEM((32, 128), f32),
            pltpu.VMEM((7, 32, 128), f32),
            dma((3,)), dma((2, mats + 1, 3)),
            dma((2,)), dma((2, ringed, 3)),
            dma((2,)), dma((2, mats)),
            dma((3,)), dma((2, mats + 1 - ringed)),
            dma((8,)), dma((8,)),
        ],
        compiler_params=pltpu.CompilerParams(
            collective_id=0, has_side_effects=True, vmem_limit_bytes=56 * 1024 * 1024
        ),
    )(traits, covariates.T, genotypes, shuffles)


def shards(traits, covariates, genotypes, shuffles):
    samples = traits.shape[0] * lax.axis_size("samp")
    out = scan(traits, covariates, genotypes, shuffles, samples)
    perms = shuffles.shape[0]
    return pl.pallas_call(
        hand_out,
        out_shape=(
            jax.ShapeDtypeStruct((32, 256), f32),
            jax.ShapeDtypeStruct((perms, 32), f32),
        ),
    )(out)


def solution(mesh):
    placed = (P("samp", None), P("samp", None), P("samp", "tile"), P(None, "samp"))
    return jax.shard_map(
        shards,
        mesh=mesh,
        in_specs=placed,
        out_specs=(P("samp", "tile"), P(None, "samp")),
        check_vma=False,
    )
```

```python
import functools
import math

import jax
import jax.numpy as jnp
from jax import lax
from jax.experimental import pallas as pl
from jax.experimental.pallas import tpu as pltpu
from jax.sharding import PartitionSpec as P

C = 32


epsilon = 1e-05
MESH = pl.DeviceIdType.MESH
f32 = jnp.float32
bf16 = jnp.bfloat16


ORDER = (
    "C0", "B", "10", "g1", "P1", "C1", "11", "P2", "C2", "201", "P4", "12",
    "P3", "C4", "14", "P5", "aux", "A1", "301", "200", "C3", "13", "210", "240",
    "A2", "241", "401", "211", "221", "C5", "230", "A3", "15", "340", "341", "310",
    "231", "311", "321", "C6", "A4", "220", "251", "g2", "16", "501", "441", "300",
    "440", "331", "421", "250", "330", "411", "260", "A5", "320", "431", "261", "g3",
    "d51", "521", "541", "540", "410", "400", "d50", "420", "511", "430", "A6", "531",
    "d61", "510", "d60", "500", "e51", "520", "530", "e50", "inv", "ct", "e61", "e60",
    "corr", "f4", "f2", "f1", "f0", "f3", "f5", "T", "f6",
)


def exact_dot(a, b):
    return jnp.dot(a, b, preferred_element_type=f32, precision=lax.Precision.HIGHEST)


def split(a):
    high = a.astype(bf16)
    rest = a - high.astype(f32)
    middle = rest.astype(bf16)
    return high, middle, (rest - middle.astype(f32)).astype(bf16)


def across(a, b):
    return lax.dot_general(a, b, (((1,), (1,)), ((), ())), preferred_element_type=f32)


def iota(shape, dim):
    return lax.broadcasted_iota(jnp.int32, shape, dim)


def scan_kernel(
    y_hbm, cov_hbm, geno_hbm, order_hbm, out_ref,
    y_ref, cov_ref, geno_ref, order_ref, load,
    yt, q, xt, tps, part, in1, mid, in2, low, inz, ind,
    apart, ain1, amid, aind, alow, alowin, agu, tt, gsum, gin,
    inv_ref, ct_ref, lhs, vst, corr, st_ref, sg_ref, pm, pmin,
    send1, recv1, send2, recv2, sendz, recvz, sendd, recvd, sendx, recvx,
    *, samples,
):
    perms = order_hbm.shape[0]
    mats = perms + 1
    own = perms
    aux = mats
    ringed = perms - 1
    rows = y_hbm.shape[0]
    s = lax.axis_index("samp")
    t = lax.axis_index("tile")
    x = lax.rem(s, 4)
    zh = lax.rem(s // 4, 2)
    y = s // 8
    core = lax.rem(t, 2)
    zl = t // 2
    base = s * rows

    def at_x(d):
        return s - x + lax.rem(x + d, 4)

    def at_y(d):
        return lax.rem(s + 8 * d, 32)

    z_peer = s + 4 - 8 * zh

    place = (x, y)
    along = (at_x, at_y)

    barrier = pltpu.get_barrier_semaphore()
    met = [at_y(d) for d in (1, 2, 3)] + [at_x(d) for d in (1, 2, 3)] + [z_peer]
    for peer in met:
        pl.semaphore_signal(barrier, inc=1, device_id={"samp": peer}, device_id_type=MESH)
    for d in range(1, 8):
        pl.semaphore_signal(
            barrier, inc=1, device_id={"tile": lax.rem(t + d, 8)}, device_id_type=MESH
        )

    loads = [
        pltpu.make_async_copy(a, b, load.at[k])
        for k, (a, b) in enumerate(
            [(cov_hbm, cov_ref), (geno_hbm, geno_ref), (order_hbm, order_ref)]
            + [(y_hbm.at[:, pl.ds(k, 256)], y_ref.at[:, pl.ds(k, 256)]) for k in range(0, 1024, 256)]
        )
    ]
    for copy in loads:
        copy.start()

    def remote(src, dst, send, recv, peer):
        return pltpu.make_async_remote_copy(
            src_ref=src, dst_ref=dst, send_sem=send, recv_sem=recv,
            device_id={"samp": peer}, device_id_type=MESH,
        )

    def to_tile(src, dst, k, d):
        return pltpu.make_async_remote_copy(
            src_ref=src, dst_ref=dst, send_sem=sendx.at[k], recv_sem=recvx.at[k],
            device_id={"tile": lax.rem(t + d, 8)}, device_id_type=MESH,
        )

    def all_of(ref, send, recv):
        return remote(ref, ref, send, recv, at_x(1))

    def ring_copy(src, buf, k, c, peers, send, recv):
        blk = lax.rem(c + (2, 2, 1, 3, 1, 3)[k], 4)
        uv = (0, 1, 1, 0, 0, 1)[k]
        ref = buf.at[k - 4] if k >= 4 else src.at[blk, uv]
        return remote(ref, buf.at[k], send, recv.at[min(k, 2)], peers((1, 3, 1, 3, 1, 3)[k]))

    def part_of(h, m):
        return apart if m == aux else part.at[h, m]

    def in1_of(h, m):
        return ain1 if m == aux else in1.at[h, m]

    def mid_of(h, m):
        return amid if m == aux else mid.at[h, m]

    def ind_of(h, m):
        return aind if m == aux else ind.at[h, m - ringed]

    def low_of(h, m):
        return alow if m == aux else low.at[h, m]

    def first_copy(h, m, k):
        return ring_copy(
            part_of(h, m), in1_of(h, m), k, place[h], along[h],
            send1.at[2 if m == aux else h], recv1.at[h, m],
        )

    def second_copy(h, m, k):
        return ring_copy(
            mid.at[h, m], in2.at[h, m], k, place[1 - h], along[1 - h], send2.at[h],
            recv2.at[h, m],
        )

    def z_copy(h, m):
        return remote(
            low.at[h, m, 1 - zh], inz.at[h, m], sendz.at[h], recvz.at[h, m], z_peer
        )

    def compute(m):
        out = jnp.dot(yt[...], q[m, :, :256], preferred_element_type=f32)
        for o in range(32):
            yb, z, xb = o // 8, o // 4 % 2, o % 4
            piece = out[o * 32 : o * 32 + 32]
            part[0, m, xb, z, yb] = piece[:, :128]
            part[1, m, yb, z, xb] = piece[:, 128:]

    def permute(m):
        order = order_ref[pl.ds(m, 1), :] - base
        hot = jnp.where(iota((rows, rows), 0) == order, 1.0, 0.0).astype(bf16)
        q[m] = jnp.dot(hot, q[own], preferred_element_type=f32).astype(bf16)

    def stage1(m, halves=(0, 1)):
        for k in range(4):
            for h in halves:
                first_copy(h, m, k).start()

    def stage2(m, halves=(0, 1)):
        for h in halves:
            c = place[h]
            lines, buf = part_of(h, m), in1_of(h, m)
            for k, d, uv in ((0, 1, 0), (1, 3, 1)):
                first_copy(h, m, k).wait_recv()
                buf[k] = buf[k] + lines[lax.rem(c + d, 4), uv]
                first_copy(h, m, k + 4).start()

    def first_sum(h, m):
        c = place[h]
        lines, buf, to = part_of(h, m), in1_of(h, m), mid_of(h, m)
        all_of(buf.at[pl.ds(2, 4)], send1.at[h], recv1.at[h, m, 2]).wait_recv()
        to[:, 0] = lines[c, 0] + buf[3] + buf[4]
        to[:, 1] = lines[c, 1] + buf[2] + buf[5]

    def stage3(m, halves=(0, 1)):
        for h in halves:
            first_sum(h, m)
            for k in range(4):
                second_copy(h, m, k).start()

    def stage4(m, halves=(0, 1)):
        for h in halves:
            c = place[1 - h]
            for k, d, uv in ((0, 1, 0), (1, 3, 1)):
                second_copy(h, m, k).wait_recv()
                in2[h, m, k] = in2[h, m, k] + mid[h, m, lax.rem(c + d, 4), uv]
                second_copy(h, m, k + 4).start()

    def stage5(m, halves=(0, 1)):
        for h in halves:
            c = place[1 - h]
            all_of(in2.at[h, m, pl.ds(2, 4)], send2.at[h], recv2.at[h, m, 2]).wait_recv()
            low[h, m, 0] = mid[h, m, c, 0] + in2[h, m, 3] + in2[h, m, 4]
            low[h, m, 1] = mid[h, m, c, 1] + in2[h, m, 2] + in2[h, m, 5]
            z_copy(h, m).start()


    def direct(m, halves=(0, 1)):
        for h in halves:
            first_sum(h, m)
            for d in (1, 3, 2):
                remote(
                    mid_of(h, m).at[lax.rem(place[1 - h] + d, 4)], ind_of(h, m).at[d - 1],
                    sendd.at[2 if m == aux else h], recvd.at[h, m - ringed], along[1 - h](d),
                ).start()

    def direct_sum(h, m):
        buf = ind_of(h, m)
        all_of(buf, sendd.at[h], recvd.at[h, m - ringed]).wait_recv()
        total = mid_of(h, m)[place[1 - h]] + buf[0] + buf[1] + buf[2]
        low_of(h, m)[...] = total

    def stage5d(m, halves=(0, 1)):
        for h in halves:
            direct_sum(h, m)
            z_copy(h, m).start()


    def spread_of(m):
        return q[m, :, 256:].astype(f32)

    def aux_parts():
        for m in range(mats):
            out = jnp.dot(xt[...], q[m, :, :256], preferred_element_type=f32)
            for j in range(4):
                for k in range(2):
                    apart[m // 2, m % 2, j, 8 + 8 * k : 16 + 8 * k] = out[
                        8 * j : 8 * j + 8, 128 * k : 128 * k + 128
                    ]
        group = iota((rows, 128), 1) // 32
        picked = []
        for k in range(2):
            value = spread_of(3) if k == 0 else jnp.where(
                iota((rows, 128), 1) == 96, 1.0, 0.0
            )
            for j in range(3):
                value = jnp.where(group == j, spread_of(4 * k + j), value)
            picked.append(value)
            out = jnp.dot(xt[...], value.astype(bf16), preferred_element_type=f32)
            for j in range(4):
                apart[3, 1, j, 8 + 8 * k : 16 + 8 * k] = out[8 * j : 8 * j + 8]
        mine = jnp.where(core == 0, picked[0], picked[1]).astype(bf16)
        out = jnp.dot(yt[...], mine, preferred_element_type=f32)
        wide = yt[...].astype(f32)
        square_at = (iota((1024, 128), 1) == 97) & (core == 1)
        out = jnp.where(square_at, jnp.sum(wide * wide, axis=1, keepdims=True), out)
        tps[...] = out.reshape(32, 32, 128)
        ours = tps[:, pl.ds(pl.multiple_of(zl * 8, 8), 8), :]
        apart[:, :, :, 0:8] = ours.reshape(4, 2, 4, 8, 128)

    def both_copy():
        return remote(alow, alowin, sendx.at[4], recvx.at[4], z_peer)

    def aux_low():
        direct_sum(1, aux)
        both_copy().start()

    def aux_total():
        both_copy().wait_recv()
        total = alow[...] + alowin[...]
        agu[x, y] = total[:, 8:]
        for d in (1, 3, 2):
            remote(agu.at[x, y], agu.at[x, y], sendx.at[2], recvx.at[2], at_y(d)).start()
        tt[t] = jnp.where(zh == 0, total[0, :8], total[1, :8])
        for d in range(1, 8):
            to_tile(tt.at[t], tt.at[t], 0, d).start()

    def aux_row():
        all_of(agu.at[x, pl.ds(0, 3)], sendx.at[2], recvx.at[2]).wait_recv()
        for d in (1, 3, 2):
            remote(agu.at[x], agu.at[x], sendx.at[3], recvx.at[3], at_x(d)).start()


    def gram_send(n):
        for d in (1, 3, 2) if n < 2 else (0,):
            peer = z_peer if n == 2 else along[n](d)
            remote(
                gsum.at[n], gin.at[3 * n + max(d - 1, 0)], sendx.at[5 + n], recvx.at[5 + n], peer
            ).start()

    def gram_start():
        lane = iota((rows, 128), 1)
        wide = jnp.where(lane < 32, spread_of(own), jnp.where(lane == 32, 1.0, 0.0))
        out = jnp.dot(xt[...], wide.astype(bf16), preferred_element_type=f32)[:40]
        geno = q[own, :, :256].astype(f32)
        row = iota((40, 128), 0)
        for k in range(2):
            half = geno[:, 128 * k : 128 * k + 128]
            out = jnp.where(row == 33 + k, jnp.sum(half, axis=0, keepdims=True), out)
            out = jnp.where(row == 35 + k, jnp.sum(half * half, axis=0, keepdims=True), out)
        gsum[0] = out
        gram_send(0)

    def gram_pass(n):
        count = 1 if n == 3 else 3
        at = 3 * n - 3
        all_of(gin.at[pl.ds(at, count)], sendx.at[4 + n], recvx.at[4 + n]).wait_recv()
        total = gsum[n - 1]
        for k in range(count):
            total = total + gin[at + k]
        gsum[n] = total
        if n < 3:
            gram_send(n)

    def invert():
        gram_pass(3)
        lane40 = iota((40, 128), 1)
        row40 = iota((40, 128), 0)
        inv = jnp.where(row40 < C + 1, gsum[3], 0.0)
        for k in range(C + 1):
            pivot = inv[k : k + 1, k : k + 1]
            line = jnp.where(lane40[:1] == k, 1.0, inv[k : k + 1, :]) / pivot
            column = inv[:, k : k + 1]
            rest = jnp.where(lane40 == k, 0.0, inv)
            inv = jnp.where(row40 == k, line, rest - column * line)
        inv_ref[:40] = inv
        inv_ref[40:] = jnp.zeros((88, 128), f32)

    def trait_side():
        all_of(tt.at[pl.ds(0, 7)], sendx.at[0], recvx.at[0]).wait_recv()
        lane = iota((32, 128), 1)
        sums = [jnp.concatenate([tt[2 * k + c] for k in range(4)], axis=0) for c in range(2)]
        ones_y = sums[1][:, 96:97]
        squares_y = sums[1][:, 97:98]
        for m in range(mats):
            mine = sums[m // 4]
            k = m % 4
            if k:
                mine = pltpu.roll(mine, 128 - 32 * k, 1)
            mine = jnp.where(lane < 32, mine, jnp.where(lane == 32, ones_y, 0.0))
            lhs[mats * 40 + m * 32 : mats * 40 + m * 32 + 32] = mine
        coef_t = exact_dot(mine, inv_ref[...])
        coef_t = coef_t.astype(bf16).astype(f32)
        ct_ref[...] = coef_t
        gram = jnp.where(iota((40, 128), 0) < C + 1, gsum[3], 0.0)
        back = exact_dot(coef_t, jnp.concatenate([gram, jnp.zeros((88, 128), f32)], axis=0))
        squares_t = squares_y - jnp.sum(coef_t * (2.0 * mine - back), axis=1, keepdims=True)
        mean_t = jnp.maximum(squares_t, 0.0) / samples
        factor_z = math.sqrt(samples - C - 2) / samples
        st_ref[...] = jnp.broadcast_to(lax.rsqrt(mean_t + epsilon) * factor_z, (32, 128))

    def corrections():
        all_of(agu.at[pl.ds(0, 3)], sendx.at[3], recvx.at[3]).wait_recv()
        lane = iota((32, 128), 1)

        def product(m, k):
            return agu[:, m // 2, m % 2, 8 * k : 8 * k + 8].reshape(32, 128)

        gram = gsum[3]
        first = iota((8, 128), 0) == 0
        last_rows = jnp.where(first, gram[32:40], 0.0)
        ones_g = jnp.concatenate([gram[33:34], gram[34:35]], axis=1)
        squares_g = jnp.concatenate([gram[35:36], gram[36:37]], axis=1)
        ones_rows = jnp.where(iota((8, 256), 0) == 0, ones_g, 0.0)
        spreads = [product(7, 0), product(7, 1)]

        def geno_of(m):
            body = jnp.concatenate([product(m, 0), product(m, 1)], axis=1)
            return jnp.concatenate([body, ones_rows], axis=0)

        for m in range(mats):
            if m == own:
                body = gram[:32]
            else:
                body = spreads[m // 4]
                if m % 4:
                    body = pltpu.roll(body, 128 - 32 * (m % 4), 1)
                body = jnp.where(lane < 32, body, jnp.where(lane == 32, gram[:32], 0.0))
            lhs[m * 40 : m * 40 + 32] = body
            lhs[m * 40 + 32 : m * 40 + 40] = last_rows
        geno0 = geno_of(own)
        pad256 = jnp.zeros((88, 256), f32)
        coef_g = exact_dot(inv_ref[:40], jnp.concatenate([geno0, pad256], axis=0))
        rounded_g = jnp.concatenate([coef_g, pad256], axis=0).astype(bf16)
        coef_g = coef_g.astype(bf16).astype(f32)
        rounded_t = ct_ref[...].astype(bf16)
        out = sum(
            jnp.dot(piece, rounded_g, preferred_element_type=f32) for piece in split(lhs[...])
        )
        for m in range(mats):
            left = geno_of(m) - out[m * 40 : m * 40 + 40]
            vst[:40, m * 256 : m * 256 + 256] = left
            vst[40:, m * 256 : m * 256 + 256] = jnp.zeros((8, 256), f32)
            if m == own:
                squares_g = squares_g - jnp.sum(
                    coef_g * (geno0 + left), axis=0, keepdims=True
                )
        more = sum(
            jnp.dot(rounded_t[:, :48], piece, preferred_element_type=f32)
            for piece in split(vst[...])
        )
        for m in range(mats):
            at = mats * 40 + m * 32
            corr[m] = out[at : at + 32] + more[:, m * 256 : m * 256 + 256]
        mean_g = jnp.maximum(squares_g, 0.0) / samples
        sg_ref[...] = jnp.broadcast_to(lax.rsqrt(mean_g + epsilon), (8, 256))

    def owned(m):
        outs = []
        for h in range(2):
            z_copy(h, m).wait_recv()
            total = low[h, m, zh] + inz[h, m]
            cols = slice(h * 128, h * 128 + 128)
            outs.append((total - corr[m, :, cols]) * sg_ref[0:1, cols])
        return outs

    loads[0].wait()
    loads[1].wait()
    spread = jnp.where(lax.rem(iota((32, 128), 1), 32) == iota((32, 128), 0), 1.0, 0.0)
    spread = spread.astype(bf16)
    for b in range(4):
        at = slice(b * 256, b * 256 + 256)
        q[own, at, :256] = geno_ref[at, :].astype(f32).astype(bf16)
        q[own, at, 256:] = lax.dot_general(
            cov_ref[:, at], spread, (((0,), (0,)), ((), ())), preferred_element_type=f32
        ).astype(bf16)
    xt[:32] = cov_ref[...]
    xt[32:] = jnp.where(iota((16, rows), 0) == 0, 1.0, 0.0).astype(bf16)
    eye = jnp.where(iota((256, 256), 0) == iota((256, 256), 1), 1.0, 0.0).astype(bf16)

    loads[2].wait()
    permute(0)
    for b in range(4):
        loads[3 + b].wait()
        at = slice(b * 256, b * 256 + 256)
        yt[at, :] = across(eye, y_ref[:, at]).astype(bf16)

    lane = iota((32, 128), 1)
    held = {"best": jnp.zeros((32, 128), f32)}

    def finish(m):
        left, right = owned(m)
        if m == own:
            out_ref[:32, :128] = left * st_ref[...]
            out_ref[:32, 128:] = right * st_ref[...]
            out_ref[32:, 128:] = jnp.zeros((8, 128), f32)
            return
        peak = jnp.max(jnp.maximum(jnp.abs(left), jnp.abs(right)), axis=1, keepdims=True)
        held["best"] = jnp.where(lane == m, peak * st_ref[...], held["best"])

    def exchange():
        pm[...] = held["best"]
        for d in range(1, 8):
            to_tile(pm, pmin.at[d - 1], 1, d).start()

    stages = {"2": stage2, "3": stage3, "4": stage4, "5": stage5, "d": direct, "e": stage5d}
    whole = {"P": permute, "C": compute, "1": stage1, "f": finish}
    single = {
        "aux": aux_parts,
        "A1": lambda: stage1(aux, (1,)),
        "A2": lambda: stage2(aux, (1,)),
        "A3": lambda: direct(aux, (1,)),
        "A4": aux_low,
        "A5": aux_total,
        "A6": aux_row,
        "inv": invert,
        "ct": trait_side,
        "corr": corrections,
        "g1": gram_start,
        "g2": lambda: gram_pass(1),
        "g3": lambda: gram_pass(2),
        "T": exchange,
        "B": lambda: pl.semaphore_wait(barrier, len(met) + 7),
    }
    for name in ORDER:
        if name in single:
            single[name]()
        elif name[0] in whole:
            whole[name[0]](int(name[1]))
        else:
            stages[name[0]](int(name[1]), (int(name[2]),))
    best = held["best"]

    for h in range(2):
        all_of(in1.at[h], send1.at[h], recv1.at[0, 0, 0]).wait_send()
        all_of(in2.at[h], send2.at[h], recv2.at[0, 0, 0]).wait_send()
        all_of(inz.at[h], sendz.at[h], recvz.at[0, 0]).wait_send()
        all_of(ind.at[h], sendd.at[h], recvd.at[0, 0]).wait_send()
    all_of(tt.at[pl.ds(0, 7)], sendx.at[0], recvx.at[0]).wait_send()
    all_of(agu.at[x, pl.ds(0, 3)], sendx.at[2], recvx.at[2]).wait_send()
    both_copy().wait_send()
    all_of(ain1, send1.at[2], recv1.at[0, 0, 0]).wait_send()
    all_of(aind, sendd.at[2], recvd.at[0, 0]).wait_send()
    for n in range(3):
        sent = gin.at[pl.ds(0, 3 if n < 2 else 1)]
        all_of(sent, sendx.at[5 + n], recvx.at[5 + n]).wait_send()
    all_of(agu.at[pl.ds(0, 3)], sendx.at[3], recvx.at[3]).wait_send()
    all_of(pmin, sendx.at[1], recvx.at[1]).wait()
    for d in range(7):
        best = jnp.maximum(best, pmin[d])
    best = jnp.concatenate([best, jnp.zeros((96, 128), f32)], axis=0)
    out_ref[32:, :128] = jnp.transpose(best)[:8]


def hand_out(both_ref, obs_ref, peak_ref):
    obs_ref[...] = both_ref[:32]
    peak_ref[...] = both_ref[32 : 32 + peak_ref.shape[0], :32]


def scan(traits, covariates, genotypes, shuffles, samples):
    perms = shuffles.shape[0]
    mats = perms + 1
    ringed = perms - 1
    rows = traits.shape[0]
    vmem = pl.BlockSpec(memory_space=pltpu.VMEM)
    dma = pltpu.SemaphoreType.DMA
    return pl.pallas_call(
        functools.partial(scan_kernel, samples=samples),
        out_shape=jax.ShapeDtypeStruct((40, 256), f32),
        in_specs=[pl.BlockSpec(memory_space=pl.ANY)] * 4,
        out_specs=vmem,
        scratch_shapes=[
            pltpu.VMEM(traits.shape, bf16),
            pltpu.VMEM(covariates.shape[::-1], bf16),
            pltpu.VMEM(genotypes.shape, jnp.int32),
            pltpu.VMEM(shuffles.shape, jnp.int32),
            dma((7,)),
            pltpu.VMEM((1024, rows), bf16),
            pltpu.VMEM((mats, rows, 384), bf16),
            pltpu.VMEM((48, rows), bf16),
            pltpu.VMEM((32, 32, 128), f32),
            pltpu.VMEM((2, mats, 4, 2, 4, 32, 128), f32),
            pltpu.VMEM((2, mats, 6, 4, 32, 128), f32),
            pltpu.VMEM((2, mats, 4, 2, 32, 128), f32),
            pltpu.VMEM((2, ringed, 6, 32, 128), f32),
            pltpu.VMEM((2, mats, 2, 32, 128), f32),
            pltpu.VMEM((2, mats, 32, 128), f32),
            pltpu.VMEM((2, mats - ringed, 3, 2, 32, 128), f32),
            pltpu.VMEM((4, 2, 4, 24, 128), f32),
            pltpu.VMEM((6, 4, 24, 128), f32),
            pltpu.VMEM((4, 2, 24, 128), f32),
            pltpu.VMEM((3, 2, 24, 128), f32),
            pltpu.VMEM((2, 24, 128), f32),
            pltpu.VMEM((2, 24, 128), f32),
            pltpu.VMEM((4, 4, 2, 16, 128), f32),
            pltpu.VMEM((8, 8, 128), f32),
            pltpu.VMEM((4, 40, 128), f32),
            pltpu.VMEM((7, 40, 128), f32),
            pltpu.VMEM((128, 128), f32),
            pltpu.VMEM((32, 128), f32),
            pltpu.VMEM((mats * 72, 128), f32),
            pltpu.VMEM((48, mats * 256), f32),
            pltpu.VMEM((mats, 32, 256), f32),
            pltpu.VMEM((32, 128), f32),
            pltpu.VMEM((8, 256), f32),
            pltpu.VMEM((32, 128), f32),
            pltpu.VMEM((7, 32, 128), f32),
            dma((3,)), dma((2, mats + 1, 3)),
            dma((2,)), dma((2, ringed, 3)),
            dma((2,)), dma((2, mats)),
            dma((3,)), dma((2, mats + 1 - ringed)),
            dma((8,)), dma((8,)),
        ],
        compiler_params=pltpu.CompilerParams(
            collective_id=0, has_side_effects=True, vmem_limit_bytes=56 * 1024 * 1024
        ),
    )(traits, covariates.T, genotypes, shuffles)


def shards(traits, covariates, genotypes, shuffles):
    samples = traits.shape[0] * lax.axis_size("samp")
    out = scan(traits, covariates, genotypes, shuffles, samples)
    perms = shuffles.shape[0]
    return pl.pallas_call(
        hand_out,
        out_shape=(
            jax.ShapeDtypeStruct((32, 256), f32),
            jax.ShapeDtypeStruct((perms, 32), f32),
        ),
    )(out)


def solution(mesh):
    placed = (P("samp", None), P("samp", None), P("samp", "tile"), P(None, "samp"))
    return jax.shard_map(
        shards,
        mesh=mesh,
        in_specs=placed,
        out_specs=(P("samp", "tile"), P(None, "samp")),
        check_vma=False,
    )
```
